128 devices in a mesh: samp: 16 (over z, y_lo, core), var: 8 (over x, y_hi).
Axes of the slice: x: 4, y: 4 (y_hi: 2, y_lo: 2; y = y_hi * 2 + y_lo), z: 4, core: 2. Of those that a mesh axis runs over, the one named last changes fastest.
Arguments:
- hap_words: int32 [2, 1024, 1024], P(None, 'samp', 'var'), may hold values from 0 to 1073741823
- total_counts: int32 [30720, 8192], P('samp', 'var'), may hold values from 0 to 4999
- allele_one: int32 [30720, 8192], P('samp', 'var'), may hold values from 0 to 299
- allele_two: int32 [30720, 8192], P('samp', 'var'), may hold values from 0 to 299
Outputs:
- z_total: float32 [1024, 8192], P('samp', 'var')
- z_allelic: float32 [1024, 8192], P('samp', 'var')
The draws below stay inside these ranges and needn't reach their ends.
Inputs may be any that keep to these rules, and one draw needn't show every extreme that they name: Bit k, for k below 30, of hap_words[c, j, v] is haplotype c of sample 30 * j + k at variant v; higher bits are zero.
All inputs are finite; a program needn't handle non-finite values.
Results may differ from the reference program's by a relative error of at most 0.0003.
The reference program's roundings to bfloat16 on the way count: a program that leaves them out, or rounds other values in their place, can miss the bound.
Values sent between devices are 32-bit elements; how exact they have to be, the bound alone decides.
No kernel may reach another device: no remote copies, remote signals or barrier semaphores. Data moves between devices by JAX's collectives and lax.ppermute only.
A program may use at most 192 MiB of HBM per device.

```python
import jax
import jax.numpy as jnp
from jax import lax

BITS = 30
GENES = 8192
SWORDS = 1024
SAMPLES = 30720
VARIANTS = 1024


def with_ends(array, own_key, low, high):
    longest = array.shape.index(max(array.shape))
    spots = []
    for shift in (0, 1):
        where = [jax.random.randint(jax.random.fold_in(own_key, axis), (), 0, length) for axis, length in enumerate(array.shape)]
        where[longest] = (where[longest] + shift) % array.shape[longest]
        spots.append(tuple(where))
    return array.at[spots[0]].set(low).at[spots[1]].set(high)


def setup_inputs(seed: int = 0) -> dict:
    seeds = jax.random.split(jax.random.key(seed), 5)
    hap_words = with_ends(jax.random.randint(seeds[0], (2, SWORDS, VARIANTS), 0, 2 ** BITS), jax.random.fold_in(seeds[0], 1), 0, (2 ** BITS) - 1).astype(jnp.int32)
    total_counts = with_ends(jax.random.randint(seeds[1], (SAMPLES, GENES), 0, 5000), jax.random.fold_in(seeds[1], 1), 0, 4999).astype(jnp.int32)
    allele_one = with_ends(jax.random.randint(seeds[2], (SAMPLES, GENES), 0, 300), jax.random.fold_in(seeds[2], 1), 0, 299).astype(jnp.int32)
    allele_two = with_ends(jax.random.randint(seeds[3], (SAMPLES, GENES), 0, 300), jax.random.fold_in(seeds[3], 1), 0, 299).astype(jnp.int32)
    return dict(hap_words=hap_words, total_counts=total_counts, allele_one=allele_one, allele_two=allele_two)


def unpack(packed):
    shifts = jnp.arange(BITS, dtype=jnp.int32)
    bit_table = jnp.bitwise_and(jnp.right_shift(packed[:, :, None, :], shifts[None, None, :, None]), 1)
    return bit_table.reshape(2, packed.shape[1] * BITS, packed.shape[2])

def features(total_part, one_part, two_part):
    log_total = jnp.log1p(total_part.astype(jnp.float32))
    one_plus = one_part.astype(jnp.float32) + 1.0
    two_plus = two_part.astype(jnp.float32) + 1.0
    log_ratio = jnp.log(one_plus / two_plus)
    weight = 1.0 / (1.0 / one_plus + 1.0 / two_plus)
    return (log_total, (weight * log_ratio).astype(jnp.bfloat16), weight.astype(jnp.bfloat16))

def finish(cross_total, cross_allelic, het_weight, dos_sum, dos_sq, gene_sum, gene_sq, sample_count):
    dosage_var = dos_sq - dos_sum * dos_sum / sample_count
    gene_var = gene_sq - gene_sum * gene_sum / sample_count
    covariance = cross_total - dos_sum[:, None] * gene_sum[None, :] / sample_count
    z_total = jnp.sqrt(sample_count) * covariance / jnp.sqrt((dosage_var[:, None] + 1.0) * (gene_var[None, :] + 1.0))
    z_allelic = cross_allelic / jnp.sqrt(het_weight + 1.0)
    return (z_total, z_allelic)

def reference(hap_words, total_counts, allele_one, allele_two):
    bit_table = unpack(hap_words)
    dosage = bit_table[0] + bit_table[1] - 1
    phase_diff = bit_table[0] - bit_table[1]
    dosage_f = dosage.astype(jnp.float32)
    dos_sum = lax.optimization_barrier(jnp.sum(dosage_f, axis=0))
    dos_sq = lax.optimization_barrier(jnp.sum(dosage_f * dosage_f, axis=0))
    dosage_b = dosage.astype(jnp.bfloat16)
    phase_b = phase_diff.astype(jnp.bfloat16)
    phase_sq_b = (phase_diff * phase_diff).astype(jnp.bfloat16)
    sample_count = jnp.float32(hap_words.shape[1] * BITS)
    block_width = GENES // 8

    def one_block(block_index):
        first_col = (block_index * block_width).astype(jnp.int32)
        total_part = lax.dynamic_slice_in_dim(total_counts, first_col, block_width, 1)
        one_part = lax.dynamic_slice_in_dim(allele_one, first_col, block_width, 1)
        two_part = lax.dynamic_slice_in_dim(allele_two, first_col, block_width, 1)
        log_total, weighted_b, weight_b = features(total_part, one_part, two_part)
        cross_total = jnp.dot(dosage_b.T, log_total.astype(jnp.bfloat16), preferred_element_type=jnp.float32)
        cross_allelic = jnp.dot(phase_b.T, weighted_b, preferred_element_type=jnp.float32)
        het_weight = jnp.dot(phase_sq_b.T, weight_b, preferred_element_type=jnp.float32)
        gene_sum = lax.optimization_barrier(jnp.sum(log_total, axis=0))
        gene_sq = lax.optimization_barrier(jnp.sum(log_total * log_total, axis=0))
        return finish(cross_total, cross_allelic, het_weight, dos_sum, dos_sq, gene_sum, gene_sq, sample_count)
    total_blocks, allelic_blocks = lax.map(one_block, jnp.arange(8, dtype=jnp.int32))
    variants = hap_words.shape[2]
    z_total = jnp.moveaxis(total_blocks, 0, 1).reshape(variants, GENES)
    z_allelic = jnp.moveaxis(allelic_blocks, 0, 1).reshape(variants, GENES)
    return (z_total, z_allelic)
```

```python
import jax
import jax.numpy as jnp
from jax import lax
from jax.experimental import pallas as pl
from jax.experimental.pallas import tpu as pltpu
from jax.sharding import PartitionSpec as P

BITS = 30
HALF = BITS // 2
LANES = 128
CHUNKS = (256, 256, 256, 256)

CORE, SIDE_Y, SIDE_A, SIDE_B = 1, 2, 4, 12
ORDERS = ((SIDE_Y, SIDE_A, SIDE_B), (SIDE_A, SIDE_B, SIDE_Y), (SIDE_B, SIDE_Y, SIDE_A))


def swap(array, axis, flip):
    size = lax.axis_size(axis)
    return lax.ppermute(array, axis, [(d, d ^ flip) for d in range(size)])


def place_of(relative, order):
    bits = {
        SIDE_Y: (relative >> 1) & 1,
        SIDE_A: ((relative >> 2) ^ (relative >> 3)) & 1,
        SIDE_B: (relative >> 3) & 1,
    }
    place = relative & 1
    for side in order:
        place = 2 * place + bits[side]
    return place


def unpack_kernel(where_ref, *refs):
    word_refs, (design_ref, margin_ref) = refs[:-2], refs[-2:]
    samp, var = where_ref[0], where_ref[1]
    low = (1 << HALF) - 1
    words, block = word_refs[0].shape[1:]
    rows = block // 2
    one, zero = jnp.bfloat16(1), jnp.bfloat16(0)
    for flip, word_ref in enumerate(word_refs):
        owner = 2 * (var ^ flip)
        first, second = word_ref[0], word_ref[1]
        ones = lax.population_count(first) + lax.population_count(second)
        mixed = lax.population_count(first ^ second)
        samples = float(words * BITS)
        margin_ref[pl.ds(var ^ flip, 1), 0:1, :] = (
            jnp.sum(ones.astype(jnp.float32), axis=0, keepdims=True) - samples
        )[None]
        margin_ref[pl.ds(var ^ flip, 1), 1:2, :] = (
            samples - jnp.sum(mixed.astype(jnp.float32), axis=0, keepdims=True)
        )[None]
        turned = [
            jnp.concatenate([w & low, (w >> HALF) & low], axis=0).T.astype(jnp.int16)
            for w in (first, second)
        ]
        for part in range(2):
            relative = (owner + part) ^ samp
            starts = [pl.multiple_of(place_of(relative, order) * rows, rows) for order in ORDERS]
            mine = [t[part * rows : (part + 1) * rows] for t in turned]
            for bit in range(HALF):
                mask = jnp.int16(1 << bit)
                hap_one = jnp.where((mine[0] & mask) != 0, one, zero)
                hap_two = jnp.where((mine[1] & mask) != 0, one, zero)
                phase = hap_one - hap_two
                lanes = slice(bit * 2 * words, (bit + 1) * 2 * words)
                design_ref[0, pl.ds(starts[0], rows), lanes] = (hap_one + hap_two) - one
                design_ref[1, pl.ds(starts[1], rows), lanes] = phase
                design_ref[2, pl.ds(starts[2], rows), lanes] = phase * phase


def unpack(where, blocks):
    _, words, block = blocks[0].shape
    variants, samples = len(blocks) * block, words * BITS
    return pl.pallas_call(
        unpack_kernel,
        out_shape=(
            jax.ShapeDtypeStruct((3, variants, samples), jnp.bfloat16),
            jax.ShapeDtypeStruct((len(blocks), 2, block), jnp.float32),
        ),
        in_specs=[pl.BlockSpec(memory_space=pltpu.SMEM)]
        + [pl.BlockSpec(memory_space=pltpu.VMEM)] * len(blocks),
        cost_estimate=pl.CostEstimate(
            flops=6_000_000_000, bytes_accessed=6 * variants * samples, transcendentals=0
        ),
        name="unpack",
    )(where, *blocks)


def feature_kernel(total_ref, one_ref, two_ref, feature_ref, margin_ref):
    words = total_ref.shape[0] // BITS

    def step(bit, sums):
        log_sum, log_sq = sums
        for half in range(2):
            rows = pl.ds(bit + half * HALF, words, stride=BITS)
            spot = pl.ds(pl.multiple_of((2 * bit + half) * words, words), words)
            log_total = jnp.log(total_ref[rows, :].astype(jnp.float32) + 1.0)
            one_plus = one_ref[rows, :].astype(jnp.float32) + 1.0
            two_plus = two_ref[rows, :].astype(jnp.float32) + 1.0
            log_ratio = jnp.log(one_plus / two_plus)
            weight = (one_plus * two_plus) / (one_plus + two_plus)
            feature_ref[0, spot, :] = log_total.astype(jnp.bfloat16)
            feature_ref[1, spot, :] = (weight * log_ratio).astype(jnp.bfloat16)
            feature_ref[2, spot, :] = weight.astype(jnp.bfloat16)
            folded = log_total.reshape(words // 8, 8, LANES)
            log_sum = log_sum + jnp.sum(folded, axis=0)
            log_sq = log_sq + jnp.sum(folded * folded, axis=0)
        return log_sum, log_sq

    blank = jnp.zeros((8, LANES), jnp.float32)
    log_sum, log_sq = lax.fori_loop(0, HALF, step, (blank, blank))
    margin_ref[0:1, :] = jnp.sum(log_sum, axis=0, keepdims=True)
    margin_ref[1:2, :] = jnp.sum(log_sq, axis=0, keepdims=True)


def features(total_counts, allele_one, allele_two, first, width):
    samples = total_counts.shape[0]
    counts = pl.BlockSpec((samples, LANES), lambda i: (0, first // LANES + i))
    return pl.pallas_call(
        feature_kernel,
        grid=(width // LANES,),
        out_shape=(
            jax.ShapeDtypeStruct((3, samples, width), jnp.bfloat16),
            jax.ShapeDtypeStruct((2, width), jnp.float32),
        ),
        in_specs=[counts, counts, counts],
        out_specs=(
            pl.BlockSpec((3, samples, LANES), lambda i: (0, 0, i)),
            pl.BlockSpec((2, LANES), lambda i: (0, i)),
        ),
        cost_estimate=pl.CostEstimate(
            flops=12_000_000 * width, bytes_accessed=18 * samples * width, transcendentals=0
        ),
        name="features",
    )(total_counts, allele_one, allele_two)


def cross_kernel(design_ref, feature_ref, keep_ref, send_ref):
    kept = keep_ref.shape[1]
    for index in range(3):
        for part, out_ref in ((1, send_ref), (0, keep_ref)):
            out_ref[index] = jnp.dot(
                design_ref[index, part * kept : (part + 1) * kept, :],
                feature_ref[index],
                preferred_element_type=jnp.float32,
            )


def cross(design, feature):
    _, variants, samples = design.shape
    width = feature.shape[2]
    part = jax.ShapeDtypeStruct((3, variants // 2, width), jnp.float32)
    return pl.pallas_call(
        cross_kernel,
        out_shape=(part, part),
        cost_estimate=pl.CostEstimate(
            flops=6 * variants * samples * width,
            bytes_accessed=6 * (variants + width) * samples,
            transcendentals=0,
        ),
        name="cross",
    )(design, feature)


def reduced(keep, send):
    got = swap(send, "samp", CORE)
    results = []
    for index, order in enumerate(ORDERS):
        current = keep[index] + got[index]
        for side in order:
            half = current.shape[0] // 2
            current = current[:half] + swap(current[half:], "samp", side)
        results.append(current)
    return results


def finish(pair_sums, dos_margin, gene_margin, sample_count):
    dos_sum, dos_sq = (dos_margin[0], dos_margin[1])
    gene_sum, gene_sq = (gene_margin[0], gene_margin[1])
    dosage_var = dos_sq - dos_sum * dos_sum / sample_count
    gene_var = gene_sq - gene_sum * gene_sum / sample_count
    covariance = pair_sums[0] - dos_sum[:, None] * gene_sum[None, :] / sample_count
    z_total = (
        jnp.sqrt(sample_count)
        * covariance
        / jnp.sqrt((dosage_var[:, None] + 1.0) * (gene_var[None, :] + 1.0))
    )
    z_allelic = pair_sums[1] / jnp.sqrt(pair_sums[2] + 1.0)
    return (z_total, z_allelic)


def per_device(hap_words, total_counts, allele_one, allele_two):
    samp, var = lax.axis_index("samp"), lax.axis_index("var")
    blocks = [hap_words] + [
        swap(hap_words, "var", flip) for flip in range(1, lax.axis_size("var"))
    ]
    design, dos_part = unpack(jnp.stack([samp, var]).astype(jnp.int32), blocks)
    sums, gene_parts = [], []
    first = 0
    for width in CHUNKS:
        feature, gene_part = features(total_counts, allele_one, allele_two, first, width)
        first += width
        sums.append(reduced(*cross(design, feature)))
        gene_parts.append(gene_part)
    variants = design.shape[1]
    genes = total_counts.shape[1]
    dos_part = jnp.moveaxis(dos_part, 1, 0).reshape(2, variants)
    margins = jnp.concatenate([*gene_parts, dos_part], axis=1)
    for side in (CORE, SIDE_Y, SIDE_A, SIDE_B):
        margins = margins + swap(margins, "samp", side)
    own = variants // lax.axis_size("samp")
    dos_margin = lax.dynamic_slice_in_dim(margins[:, genes:], samp * own, own, 1)
    sample_count = jnp.float32(total_counts.shape[0] * lax.axis_size("samp"))
    outs, first = [], 0
    for pair_sums, width in zip(sums, CHUNKS):
        outs.append(finish(pair_sums, dos_margin, margins[:, first : first + width], sample_count))
        first += width
    return tuple(jnp.concatenate(parts, axis=1) for parts in zip(*outs))


def solution(mesh):
    in_specs = (P(None, "samp", "var"), P("samp", "var"), P("samp", "var"), P("samp", "var"))
    out_specs = (P("samp", "var"), P("samp", "var"))
    return jax.shard_map(
        per_device, mesh=mesh, in_specs=in_specs, out_specs=out_specs, check_vma=False
    )
```

```python
import jax
import jax.numpy as jnp
from jax import lax
from jax.experimental import pallas as pl
from jax.experimental.pallas import tpu as pltpu
from jax.sharding import PartitionSpec as P

BITS = 30
HALF = BITS // 2
LANES = 128
CHUNKS = (512, 512)
MIB = 1024 * 1024

CORE, SIDE_Y, SIDE_A, SIDE_B = 1, 2, 4, 12
MARGIN_ORDER = (CORE, SIDE_Y, SIDE_A, SIDE_B)
ORDERS = ((SIDE_Y, SIDE_A, SIDE_B), (SIDE_A, SIDE_B, SIDE_Y), (SIDE_B, SIDE_Y, SIDE_A))


def swap(array, axis, flip):
    size = lax.axis_size(axis)
    return lax.ppermute(array, axis, [(d, d ^ flip) for d in range(size)])


def place_of(relative, order):
    bits = {
        SIDE_Y: (relative >> 1) & 1,
        SIDE_A: ((relative >> 2) ^ (relative >> 3)) & 1,
        SIDE_B: (relative >> 3) & 1,
    }
    place = relative & 1
    for side in order:
        place = 2 * place + bits[side]
    return place


def unpack_kernel(where_ref, own_ref, twin_ref, *refs):
    far_refs, (dosage_ref, phase_ref, mixed_ref, margin_ref) = refs[:-4], refs[-4:]
    samp, var = where_ref[0], where_ref[1]
    low = (1 << HALF) - 1
    words, block = own_ref.shape[1:]
    rows = block // 2
    samples = float(words * BITS)
    one, zero = jnp.bfloat16(1), jnp.bfloat16(0)
    pieces = [(0, own_ref, 0), (1, twin_ref, 0)]
    for step, far_ref in enumerate(far_refs):
        pieces += [(2 * step + 2 + twin, far_ref, 2 * twin) for twin in range(2)]
    for flip, word_ref, spot in pieces:
        source = var ^ flip
        first, second = word_ref[spot], word_ref[spot + 1]
        ones = lax.population_count(first) + lax.population_count(second)
        mixed = lax.population_count(first ^ second)
        margin_ref[pl.ds(source, 1), 0:1, :] = (
            jnp.sum(ones.astype(jnp.float32), axis=0, keepdims=True) - samples
        )[None]
        margin_ref[pl.ds(source, 1), 1:2, :] = (
            samples - jnp.sum(mixed.astype(jnp.float32), axis=0, keepdims=True)
        )[None]
        turned = [
            jnp.concatenate([w & low, (w >> HALF) & low], axis=0).T.astype(jnp.int16)
            for w in (first, second)
        ]
        for part in range(2):
            relative = (2 * source + part) ^ samp
            starts = [pl.multiple_of(place_of(relative, order) * rows, rows) for order in ORDERS]
            mine = [t[part * rows : (part + 1) * rows] for t in turned]
            for bit in range(HALF):
                mask = jnp.int16(1 << bit)
                hap_one = jnp.where((mine[0] & mask) != 0, one, zero)
                hap_two = jnp.where((mine[1] & mask) != 0, one, zero)
                phase = hap_one - hap_two
                lanes = slice(bit * 2 * words, (bit + 1) * 2 * words)
                dosage_ref[pl.ds(starts[0], rows), lanes] = (hap_one + hap_two) - one
                phase_ref[pl.ds(starts[1], rows), lanes] = phase
                mixed_ref[pl.ds(starts[2], rows), lanes] = phase * phase


def unpack(where, own, twin, far):
    _, words, block = own.shape
    count = 2 + 2 * len(far)
    variants, samples = count * block, words * BITS
    design = jax.ShapeDtypeStruct((variants, samples), jnp.bfloat16)
    return pl.pallas_call(
        unpack_kernel,
        out_shape=(design,) * 3 + (jax.ShapeDtypeStruct((count, 2, block), jnp.float32),),
        in_specs=[pl.BlockSpec(memory_space=pltpu.SMEM)]
        + [pl.BlockSpec(memory_space=pltpu.VMEM)] * (2 + len(far)),
        cost_estimate=pl.CostEstimate(
            flops=6_000_000_000, bytes_accessed=6 * variants * samples, transcendentals=0
        ),
        compiler_params=pltpu.CompilerParams(vmem_limit_bytes=8 * MIB),
        name="unpack",
    )(where, own, twin, *far)


def feature_kernel(total_ref, one_ref, two_ref, *refs):
    total_out, weighted_out, weight_out, margin_ref = refs[-4:]
    words = total_ref.shape[0] // BITS

    def step(bit, sums):
        log_sum, log_sq = sums
        for half in range(2):
            rows = pl.ds(bit + half * HALF, words, stride=BITS)
            spot = pl.ds(pl.multiple_of((2 * bit + half) * words, words), words)
            log_total = jnp.log(total_ref[rows, :].astype(jnp.float32) + 1.0)
            one_plus = one_ref[rows, :].astype(jnp.float32) + 1.0
            two_plus = two_ref[rows, :].astype(jnp.float32) + 1.0
            log_ratio = jnp.log(one_plus / two_plus)
            weight = (one_plus * two_plus) / (one_plus + two_plus)
            total_out[0, spot, :] = log_total.astype(jnp.bfloat16)
            weighted_out[0, spot, :] = (weight * log_ratio).astype(jnp.bfloat16)
            weight_out[0, spot, :] = weight.astype(jnp.bfloat16)
            folded = log_total.reshape(words // 8, 8, LANES)
            log_sum = log_sum + jnp.sum(folded, axis=0)
            log_sq = log_sq + jnp.sum(folded * folded, axis=0)
        return log_sum, log_sq

    blank = jnp.zeros((8, LANES), jnp.float32)
    log_sum, log_sq = lax.fori_loop(0, HALF, step, (blank, blank))
    margin_ref[0:1, :] = jnp.sum(log_sum, axis=0, keepdims=True)
    margin_ref[1:2, :] = jnp.sum(log_sq, axis=0, keepdims=True)


def features(total_counts, allele_one, allele_two, first, width, after):
    samples = total_counts.shape[0]
    counts = pl.BlockSpec((samples, LANES), lambda i: (0, first // LANES + i))
    feature = jax.ShapeDtypeStruct((width // LANES, samples, LANES), jnp.bfloat16)
    return pl.pallas_call(
        feature_kernel,
        grid=(width // LANES,),
        out_shape=(feature,) * 3 + (jax.ShapeDtypeStruct((2, width), jnp.float32),),
        in_specs=[counts] * 3 + [pl.BlockSpec(memory_space=pl.ANY)] * len(after),
        out_specs=(pl.BlockSpec((1, samples, LANES), lambda i: (i, 0, 0)),) * 3
        + (pl.BlockSpec((2, LANES), lambda i: (0, i)),),
        cost_estimate=pl.CostEstimate(
            flops=12_000_000 * width, bytes_accessed=18 * samples * width, transcendentals=0
        ),
        compiler_params=pltpu.CompilerParams(vmem_limit_bytes=46 * MIB),
        name="features",
    )(total_counts, allele_one, allele_two, *after)


def cross_kernel(design_ref, feature_ref, *refs):
    keep_ref, send_ref = refs[-2:]
    kept = keep_ref.shape[0]
    for pair in range(feature_ref.shape[0] // 2):
        right = jnp.concatenate([feature_ref[2 * pair], feature_ref[2 * pair + 1]], axis=1)
        lanes = slice(pair * 2 * LANES, (pair + 1) * 2 * LANES)
        for part, out_ref in ((1, send_ref), (0, keep_ref)):
            out_ref[:, lanes] = jnp.dot(
                design_ref[part * kept : (part + 1) * kept, :],
                right,
                preferred_element_type=jnp.float32,
            )


def cross(design, feature, after):
    variants, samples = design.shape
    width = feature.shape[0] * LANES
    part = jax.ShapeDtypeStruct((variants // 2, width), jnp.float32)
    return pl.pallas_call(
        cross_kernel,
        out_shape=(part, part),
        in_specs=[pl.BlockSpec(memory_space=pltpu.VMEM)] * 2
        + [pl.BlockSpec(memory_space=pl.ANY)] * len(after),
        cost_estimate=pl.CostEstimate(
            flops=2 * variants * samples * width,
            bytes_accessed=2 * (variants + width) * samples,
            transcendentals=0,
        ),
        compiler_params=pltpu.CompilerParams(vmem_limit_bytes=8 * MIB),
        name="cross",
    )(design, feature, *after)


def fold_kernel(left_ref, right_ref, keep_ref, send_ref):
    half = keep_ref.shape[0]
    keep_ref[...] = left_ref[:half] + right_ref[:half]
    send_ref[...] = left_ref[half:] + right_ref[half:]


def fold(left, right):
    rows, width = left.shape
    part = jax.ShapeDtypeStruct((rows // 2, width), jnp.float32)
    return pl.pallas_call(
        fold_kernel,
        out_shape=(part, part),
        cost_estimate=pl.CostEstimate(
            flops=rows * width, bytes_accessed=12 * rows * width, transcendentals=0
        ),
        compiler_params=pltpu.CompilerParams(vmem_limit_bytes=8 * MIB),
        name="fold",
    )(left, right)


def finish(pair_sums, dos_margin, gene_margin, sample_count):
    dos_sum, dos_sq = (dos_margin[0], dos_margin[1])
    gene_sum, gene_sq = (gene_margin[0], gene_margin[1])
    dosage_var = dos_sq - dos_sum * dos_sum / sample_count
    gene_var = gene_sq - gene_sum * gene_sum / sample_count
    covariance = pair_sums[0] - dos_sum[:, None] * gene_sum[None, :] / sample_count
    z_total = (
        jnp.sqrt(sample_count)
        * covariance
        / jnp.sqrt((dosage_var[:, None] + 1.0) * (gene_var[None, :] + 1.0))
    )
    z_allelic = pair_sums[1] / jnp.sqrt(pair_sums[2] + 1.0)
    return (z_total, z_allelic)


def per_device(hap_words, total_counts, allele_one, allele_two):
    samp, var = lax.axis_index("samp"), lax.axis_index("var")
    twin = swap(hap_words, "var", 1)
    counts = (total_counts, allele_one, allele_two)
    starts = [sum(CHUNKS[:chunk]) for chunk in range(len(CHUNKS))]
    made = []
    for chunk, (start, width) in enumerate(zip(starts, CHUNKS)):
        made.append(features(*counts, start, width, () if chunk == 0 else (twin,)))
    pair = jnp.concatenate([hap_words, twin], axis=0)
    far = []
    for flip in (2, 4, 6):
        far.append(swap(pair, "var", flip))
    *designs, dos_part = unpack(jnp.stack([samp, var]).astype(jnp.int32), hap_words, twin, far)
    sums, first_sends = [], [()] * 3
    for feature in made:
        folded = []
        for index in range(3):
            keep, send = cross(designs[index], feature[index], first_sends[index])
            got = swap(send, "samp", CORE)
            folded.append(fold(keep, got))
        first_sends = [(send,) for _, send in folded]
        for step in range(3):
            got = []
            for index in range(3):
                got.append(swap(folded[index][1], "samp", ORDERS[index][step]))
            if step < 2:
                folded = [fold(folded[i][0], got[i]) for i in range(3)]
            else:
                sums.append([folded[i][0] + got[i] for i in range(3)])
    gene_parts = [parts[3] for parts in made]
    variants = designs[0].shape[0]
    genes = total_counts.shape[1]
    dos_part = jnp.moveaxis(dos_part, 1, 0).reshape(2, variants)
    margins = jnp.concatenate([*gene_parts, dos_part], axis=1)
    margins, *_ = lax.optimization_barrier((margins, *first_sends))
    for side in MARGIN_ORDER:
        got = swap(margins, "samp", side)
        margins = margins + got
    own = variants // lax.axis_size("samp")
    dos_margin = lax.dynamic_slice_in_dim(margins[:, genes:], samp * own, own, 1)
    sample_count = jnp.float32(total_counts.shape[0] * lax.axis_size("samp"))
    outs, first = [], 0
    for pair_sums, width in zip(sums, CHUNKS):
        outs.append(finish(pair_sums, dos_margin, margins[:, first : first + width], sample_count))
        first += width
    return tuple(jnp.concatenate(parts, axis=1) for parts in zip(*outs))


def solution(mesh):
    in_specs = (P(None, "samp", "var"), P("samp", "var"), P("samp", "var"), P("samp", "var"))
    out_specs = (P("samp", "var"), P("samp", "var"))

    return jax.shard_map(
        per_device, mesh=mesh, in_specs=in_specs, out_specs=out_specs, check_vma=False
    )
```

```python
import functools

import jax
import jax.numpy as jnp
from jax import lax
from jax.experimental import pallas as pl
from jax.experimental.pallas import tpu as pltpu
from jax.sharding import PartitionSpec as P

BITS = 30
HALF = BITS // 2
LANES = 128
MIB = 1024 * 1024
MADE = (2, 6)
CHUNKS = (2, 4, 2)
GROUPS = ((0, 1), (2,))
DOS_CHUNK = 1
EXTRA = 8

CORE, SIDE_Y, SIDE_A, SIDE_B = 1, 2, 4, 12
ORDERS = ((SIDE_Y, SIDE_A, SIDE_B), (SIDE_A, SIDE_B, SIDE_Y), (SIDE_B, SIDE_Y, SIDE_A))


def swap(array, axis, flip):
    size = lax.axis_size(axis)
    return lax.ppermute(array, axis, [(d, d ^ flip) for d in range(size)])


def place_of(relative, order):
    bits = {
        SIDE_Y: (relative >> 1) & 1,
        SIDE_A: ((relative >> 2) ^ (relative >> 3)) & 1,
        SIDE_B: (relative >> 3) & 1,
    }
    place = relative & 1
    for side in order:
        place = 2 * place + bits[side]
    return place


def whole(count):
    return [pl.BlockSpec(memory_space=pltpu.VMEM)] * count


def params(mib):
    return pltpu.CompilerParams(vmem_limit_bytes=mib * MIB)


def unpack_kernel(where_ref, own_ref, twin_ref, *refs):
    far_refs, (dosage_ref, phase_ref, mixed_ref, margin_ref) = refs[:-4], refs[-4:]
    samp, var = where_ref[0], where_ref[1]
    low = (1 << HALF) - 1
    words, block = own_ref.shape[1:]
    rows = block // 2
    samples = float(words * BITS)
    one, zero = jnp.bfloat16(1), jnp.bfloat16(0)
    pieces = [(0, own_ref, 0), (1, twin_ref, 0)]
    for step, far_ref in enumerate(far_refs):
        pieces += [(2 * step + 2 + twin, far_ref, 2 * twin) for twin in range(2)]
    for flip, word_ref, spot in pieces:
        source = var ^ flip
        first, second = word_ref[spot], word_ref[spot + 1]
        ones = lax.population_count(first) + lax.population_count(second)
        mixed = lax.population_count(first ^ second)
        margin_ref[pl.ds(source, 1), 0:1, :] = (
            jnp.sum(ones.astype(jnp.float32), axis=0, keepdims=True) - samples
        )[None]
        margin_ref[pl.ds(source, 1), 1:2, :] = (
            samples - jnp.sum(mixed.astype(jnp.float32), axis=0, keepdims=True)
        )[None]
        turned = [
            jnp.concatenate([w & low, (w >> HALF) & low], axis=0).T.astype(jnp.int16)
            for w in (first, second)
        ]
        for part in range(2):
            relative = (2 * source + part) ^ samp
            starts = [pl.multiple_of(place_of(relative, order) * rows, rows) for order in ORDERS]
            mine = [t[part * rows : (part + 1) * rows] for t in turned]
            for bit in range(HALF):
                mask = jnp.int16(1 << bit)
                hap_one = jnp.where((mine[0] & mask) != 0, one, zero)
                hap_two = jnp.where((mine[1] & mask) != 0, one, zero)
                phase = hap_one - hap_two
                lanes = slice(bit * 2 * words, (bit + 1) * 2 * words)
                dosage_ref[pl.ds(starts[0], rows), lanes] = (hap_one + hap_two) - one
                phase_ref[pl.ds(starts[1], rows), lanes] = phase
                mixed_ref[pl.ds(starts[2], rows), lanes] = phase * phase


def unpack(where, own, twin, far):
    _, words, block = own.shape
    count = 2 + 2 * len(far)
    variants, samples = count * block, words * BITS
    design = jax.ShapeDtypeStruct((variants, samples), jnp.bfloat16)
    return pl.pallas_call(
        unpack_kernel,
        out_shape=(design,) * 3 + (jax.ShapeDtypeStruct((count, 2, block), jnp.float32),),
        in_specs=[pl.BlockSpec(memory_space=pltpu.SMEM)] + whole(2 + len(far)),
        cost_estimate=pl.CostEstimate(
            flops=6_000_000_000, bytes_accessed=6 * variants * samples, transcendentals=0
        ),
        compiler_params=params(8),
        name="unpack",
    )(where, own, twin, *far)


def feature_kernel(first, total_hbm, one_hbm, two_hbm, *refs):
    total_out, weighted_out, weight_out, margin_ref, buffer, sems = refs[-6:]
    blocks, samples = total_out.shape[:2]
    words = samples // BITS

    def copies(block):
        lanes = pl.ds((first + block) * LANES, LANES)
        return [
            pltpu.make_async_copy(ref.at[:, lanes], buffer.at[spot, block], sems.at[spot, block])
            for spot, ref in enumerate((total_hbm, one_hbm, two_hbm))
        ]

    for block in range(blocks):
        for copy in copies(block):
            copy.start()
    for block in range(blocks):
        for copy in copies(block):
            copy.wait()

        def step(bit, sums, block=block):
            log_sum, log_sq = sums
            for half in range(2):
                rows = pl.ds(bit + half * HALF, words, stride=BITS)
                spot = pl.ds(pl.multiple_of((2 * bit + half) * words, words), words)
                log_total = jnp.log(buffer[0, block, rows, :].astype(jnp.float32) + 1.0)
                one_plus = buffer[1, block, rows, :].astype(jnp.float32) + 1.0
                two_plus = buffer[2, block, rows, :].astype(jnp.float32) + 1.0
                log_ratio = jnp.log(one_plus / two_plus)
                weight = (one_plus * two_plus) / (one_plus + two_plus)
                total_out[block, spot, :] = log_total.astype(jnp.bfloat16)
                weighted_out[block, spot, :] = (weight * log_ratio).astype(jnp.bfloat16)
                weight_out[block, spot, :] = weight.astype(jnp.bfloat16)
                folded = log_total.reshape(words // 8, 8, LANES)
                log_sum = log_sum + jnp.sum(folded, axis=0)
                log_sq = log_sq + jnp.sum(folded * folded, axis=0)
            return log_sum, log_sq

        blank = jnp.zeros((8, LANES), jnp.float32)
        sums = lax.fori_loop(0, HALF, step, (blank, blank), unroll=3)
        for kind in range(2):
            margin_ref[kind : kind + 1, block * LANES : (block + 1) * LANES] = jnp.sum(
                sums[kind], axis=0, keepdims=True
            )


def features(total_counts, allele_one, allele_two, first, blocks, after):
    samples = total_counts.shape[0]
    width = blocks * LANES
    feature = jax.ShapeDtypeStruct((blocks, samples, LANES), jnp.bfloat16)
    return pl.pallas_call(
        functools.partial(feature_kernel, first),
        out_shape=(feature,) * 3 + (jax.ShapeDtypeStruct((2, width), jnp.float32),),
        in_specs=[pl.BlockSpec(memory_space=pltpu.HBM)] * 3
        + [pl.BlockSpec(memory_space=pl.ANY)] * len(after),
        out_specs=tuple(whole(4)),
        scratch_shapes=[
            pltpu.VMEM((3, blocks, samples, LANES), jnp.int32),
            pltpu.SemaphoreType.DMA((3, blocks)),
        ],
        cost_estimate=pl.CostEstimate(
            flops=12_000_000 * width, bytes_accessed=18 * samples * width, transcendentals=0
        ),
        compiler_params=params(44),
        name="features",
    )(total_counts, allele_one, allele_two, *after)


def cross_kernel(spots, margins, design_ref, *refs):
    keep_ref, send_ref = refs[-2:]
    calls = 1 + max(call for call, _ in spots)
    feature_refs, margin_refs = refs[:calls], refs[calls : calls + margins]
    kept = design_ref.shape[0] // 2
    for pair in range(len(spots) // 2):
        right = jnp.concatenate(
            [feature_refs[call][block] for call, block in spots[2 * pair : 2 * pair + 2]], axis=1
        )
        lanes = slice(pair * 2 * LANES, (pair + 1) * 2 * LANES)
        for part, out_ref in ((1, send_ref), (0, keep_ref)):
            out_ref[:kept, lanes] = jnp.dot(
                design_ref[part * kept : (part + 1) * kept, :],
                right,
                preferred_element_type=jnp.float32,
            )
    if margins:
        blank = jnp.zeros((EXTRA - 2, LANES), jnp.float32)
        for place, (call, block) in enumerate(spots):
            gene = margin_refs[call][:, block * LANES : (block + 1) * LANES]
            rest = blank
            if margins > calls:
                dos_ref = margin_refs[calls]
                picked = [
                    dos_ref[spot // 2, spot % 2 : spot % 2 + 1, :]
                    for spot in range(place, 2 * dos_ref.shape[0], len(spots))
                ]
                rest = jnp.concatenate([*picked, blank[len(picked) :]], axis=0)
            rows = jnp.concatenate([gene, rest], axis=0)
            lanes = slice(place * LANES, (place + 1) * LANES)
            keep_ref[kept:, lanes] = rows
            send_ref[kept:, lanes] = rows


def cross(design, features_of, spots, margins, after):
    variants, samples = design.shape
    width = len(spots) * LANES
    rows = variants // 2 + (EXTRA if margins else 0)
    part = jax.ShapeDtypeStruct((rows, width), jnp.float32)
    return pl.pallas_call(
        functools.partial(cross_kernel, spots, len(margins)),
        out_shape=(part, part),
        in_specs=whole(1 + len(features_of) + len(margins))
        + [pl.BlockSpec(memory_space=pl.ANY)] * len(after),
        cost_estimate=pl.CostEstimate(
            flops=2 * variants * samples * width,
            bytes_accessed=2 * (variants + width) * samples,
            transcendentals=0,
        ),
        compiler_params=params(8),
        name="cross",
    )(design, *features_of, *margins, *after)


def fold_kernel(extra, *refs):
    keep_ref, send_ref = refs[-2:]
    count = (len(refs) - 2) // 2
    half = keep_ref.shape[0] - extra
    first = 0
    for left_ref, right_ref in zip(refs[:count], refs[count : 2 * count]):
        lanes = slice(first, first + left_ref.shape[1])
        first += left_ref.shape[1]
        keep_ref[:half, lanes] = left_ref[:half] + right_ref[:half]
        send_ref[:half, lanes] = left_ref[half : 2 * half] + right_ref[half : 2 * half]
        if extra:
            margin = left_ref[2 * half :] + right_ref[2 * half :]
            keep_ref[half:, lanes] = margin
            send_ref[half:, lanes] = margin


def fold(lefts, rights, extra):
    half = (lefts[0].shape[0] - extra) // 2
    width = sum(left.shape[1] for left in lefts)
    part = jax.ShapeDtypeStruct((half + extra, width), jnp.float32)
    return pl.pallas_call(
        functools.partial(fold_kernel, extra),
        out_shape=(part, part),
        in_specs=whole(2 * len(lefts)),
        cost_estimate=pl.CostEstimate(
            flops=2 * half * width, bytes_accessed=24 * half * width, transcendentals=0
        ),
        compiler_params=params(8),
        name="fold",
    )(*lefts, *rights)


def finish_kernel(sample_count, dos_first, dos_blocks, where_ref, *refs):
    left_refs, right_refs, (total_ref, allelic_ref) = refs[:3], refs[3:6], refs[6:]
    own = total_ref.shape[0]
    samp = where_ref[0]
    margin = left_refs[0][own:, :] + right_refs[0][own:, :]
    columns = []
    for kind in range(2):
        picked = jnp.zeros((1, LANES), jnp.float32)
        for source in range(lax.axis_size("var")):
            spot = 2 * source + kind
            row, block = 2 + spot // dos_blocks, dos_first + spot % dos_blocks
            row_now = margin[row : row + 1, block * LANES : (block + 1) * LANES]
            picked = jnp.where(samp >> 1 == source, row_now, picked)
        turned = jnp.broadcast_to(picked, (LANES, LANES)).T
        columns.append(jnp.where(samp & 1 == 0, turned[:own], turned[own:]))
    dos_sum, dos_sq = columns
    dosage_var = dos_sq - dos_sum * dos_sum / sample_count
    scale = jnp.sqrt(jnp.float32(sample_count))
    for block in range(total_ref.shape[1] // LANES):
        lanes = slice(block * LANES, (block + 1) * LANES)
        gene_sum, gene_sq = margin[0:1, lanes], margin[1:2, lanes]
        gene_var = gene_sq - gene_sum * gene_sum / sample_count
        pair_sums = [
            left_ref[:own, lanes] + right_ref[:own, lanes]
            for left_ref, right_ref in zip(left_refs, right_refs)
        ]
        covariance = pair_sums[0] - dos_sum * gene_sum / sample_count
        total_ref[:, lanes] = (
            scale * covariance / jnp.sqrt((dosage_var + 1.0) * (gene_var + 1.0))
        )
        allelic_ref[:, lanes] = pair_sums[1] / jnp.sqrt(pair_sums[2] + 1.0)


def finish(where, lefts, rights, sample_count):
    own, width = lefts[1].shape
    dos_first = sum(CHUNKS[:DOS_CHUNK])
    out = jax.ShapeDtypeStruct((own, width), jnp.float32)
    return pl.pallas_call(
        functools.partial(finish_kernel, sample_count, dos_first, CHUNKS[DOS_CHUNK]),
        out_shape=(out, out),
        in_specs=[pl.BlockSpec(memory_space=pltpu.SMEM)] + whole(6),
        compiler_params=params(8),
        name="finish",
    )(where, *lefts, *rights)


def per_device(hap_words, total_counts, allele_one, allele_two):
    where = jnp.stack([lax.axis_index("samp"), lax.axis_index("var")]).astype(jnp.int32)
    twin = swap(hap_words, "var", 1)
    counts = (total_counts, allele_one, allele_two)
    made = []
    for call, blocks in enumerate(MADE):
        first = sum(MADE[:call])
        made.append(features(*counts, first, blocks, (twin,) if call else ()))
    pair = jnp.concatenate([hap_words, twin], axis=0)
    far = []
    for flip in (2, 4, 6):
        far.append(swap(pair, "var", flip))
    *designs, dos_part = unpack(where, hap_words, twin, far)
    spots = [(call, block) for call, blocks in enumerate(MADE) for block in range(blocks)]
    extras = (EXTRA, 0, 0)
    lefts = [[] for _ in range(3)]
    rights = [[] for _ in range(3)]
    waits = [()] * 3
    for chunk, blocks in enumerate(CHUNKS):
        first = sum(CHUNKS[:chunk])
        mine = spots[first : first + blocks]
        calls = 1 + max(call for call, _ in mine)
        for index in range(3):
            margins = [made[call][3] for call in range(calls)] if index == 0 else []
            if margins and chunk == DOS_CHUNK:
                margins.append(dos_part)
            keep, send = cross(
                designs[index],
                [made[call][index] for call in range(calls)],
                mine,
                margins,
                waits[index],
            )
            got = swap(send, "samp", CORE)
            keep, send = fold([keep], [got], extras[index])
            waits[index] = (send,)
            lefts[index].append(keep)
            rights[index].append(swap(send, "samp", ORDERS[index][0]))
    for groups, step in ((GROUPS, 1), ((range(len(GROUPS)),), 2)):
        new_lefts = [[] for _ in range(3)]
        new_rights = [[] for _ in range(3)]
        for group in groups:
            for index in range(3):
                keep, send = fold(
                    [lefts[index][g] for g in group],
                    [rights[index][g] for g in group],
                    extras[index],
                )
                new_lefts[index].append(keep)
                new_rights[index].append(swap(send, "samp", ORDERS[index][step]))
        lefts, rights = new_lefts, new_rights
    sample_count = float(total_counts.shape[0] * lax.axis_size("samp"))
    return finish(
        where, [left[0] for left in lefts], [right[0] for right in rights], sample_count
    )


def solution(mesh):
    in_specs = (P(None, "samp", "var"), P("samp", "var"), P("samp", "var"), P("samp", "var"))
    out_specs = (P("samp", "var"), P("samp", "var"))

    return jax.shard_map(
        per_device, mesh=mesh, in_specs=in_specs, out_specs=out_specs, check_vma=False
    )
```

```python
import functools

import jax
import jax.numpy as jnp
from jax import lax
from jax.experimental import pallas as pl
from jax.experimental.pallas import tpu as pltpu
from jax.sharding import PartitionSpec as P

BITS = 30
HALF = BITS // 2
LANES = 128
MIB = 1024 * 1024
MADE = (2, 6)
CHUNKS = (4, 4)
DOS_CHUNK = 0
EXTRA = 8

CORE, SIDE_Y, SIDE_A, SIDE_B = 1, 2, 4, 12
ORDERS = ((SIDE_Y, SIDE_A, SIDE_B), (SIDE_A, SIDE_B, SIDE_Y), (SIDE_B, SIDE_Y, SIDE_A))
TURNED = ((1, 1),)
FAR = (4, 2, 6)


def swap(array, axis, flip):
    size = lax.axis_size(axis)
    return lax.ppermute(array, axis, [(d, d ^ flip) for d in range(size)])


def place_of(relative, order):
    bits = {
        SIDE_Y: (relative >> 1) & 1,
        SIDE_A: ((relative >> 2) ^ (relative >> 3)) & 1,
        SIDE_B: (relative >> 3) & 1,
    }
    first, second, third = order
    return 8 * bits[first] + 4 * (relative & 1) + 2 * bits[second] + bits[third]


def sides(index, chunk):
    first, second, third = ORDERS[index]
    return (first, third, second) if (index, chunk) in TURNED else (first, second, third)


def whole(count):
    return [pl.BlockSpec(memory_space=pltpu.VMEM)] * count


def params(mib):
    return pltpu.CompilerParams(vmem_limit_bytes=mib * MIB)


def unpack_kernel(where_ref, *refs):
    word_refs, (dosage_ref, phase_ref, mixed_ref, margin_ref) = refs[:-4], refs[-4:]
    samp, var = where_ref[0], where_ref[1]
    low = (1 << HALF) - 1
    words, block = word_refs[0].shape[1:]
    rows = block // 2
    samples = float(words * BITS)
    one, zero = jnp.bfloat16(1), jnp.bfloat16(0)
    pieces = [
        (flip + twin, word_ref, 2 * twin)
        for flip, word_ref in zip((0, *FAR), word_refs)
        for twin in range(2)
    ]
    for flip, word_ref, spot in pieces:
        source = var ^ flip
        first, second = word_ref[spot], word_ref[spot + 1]
        ones = lax.population_count(first) + lax.population_count(second)
        mixed = lax.population_count(first ^ second)
        margin_ref[pl.ds(source, 1), 0:1, :] = (
            jnp.sum(ones.astype(jnp.float32), axis=0, keepdims=True) - samples
        )[None]
        margin_ref[pl.ds(source, 1), 1:2, :] = (
            samples - jnp.sum(mixed.astype(jnp.float32), axis=0, keepdims=True)
        )[None]
        turned = [
            jnp.concatenate([w & low, (w >> HALF) & low], axis=0).T.astype(jnp.int16)
            for w in (first, second)
        ]
        for part in range(2):
            relative = (2 * source + part) ^ samp
            starts = [pl.multiple_of(place_of(relative, order) * rows, rows) for order in ORDERS]
            mine = [t[part * rows : (part + 1) * rows] for t in turned]
            for bit in range(HALF):
                mask = jnp.int16(1 << bit)
                hap_one = jnp.where((mine[0] & mask) != 0, one, zero)
                hap_two = jnp.where((mine[1] & mask) != 0, one, zero)
                phase = hap_one - hap_two
                lanes = slice(bit * 2 * words, (bit + 1) * 2 * words)
                dosage_ref[pl.ds(starts[0], rows), lanes] = (hap_one + hap_two) - one
                phase_ref[pl.ds(starts[1], rows), lanes] = phase
                mixed_ref[pl.ds(starts[2], rows), lanes] = phase * phase


def unpack(where, pairs):
    _, words, block = pairs[0].shape
    count = 2 * len(pairs)
    variants, samples = count * block, words * BITS
    design = jax.ShapeDtypeStruct((variants, samples), jnp.bfloat16)
    return pl.pallas_call(
        unpack_kernel,
        out_shape=(design,) * 3 + (jax.ShapeDtypeStruct((count, 2, block), jnp.float32),),
        in_specs=[pl.BlockSpec(memory_space=pltpu.SMEM)] + whole(len(pairs)),
        cost_estimate=pl.CostEstimate(
            flops=6_000_000_000, bytes_accessed=6 * variants * samples, transcendentals=0
        ),
        compiler_params=params(8),
        name="unpack",
    )(where, *pairs)


def pair_kernel(own_ref, twin_ref, pair_ref):
    pair_ref[:2] = own_ref[...]
    pair_ref[2:] = twin_ref[...]


def paired(own, twin):
    _, words, block = own.shape
    return pl.pallas_call(
        pair_kernel,
        out_shape=jax.ShapeDtypeStruct((4, words, block), own.dtype),
        in_specs=whole(2),
        compiler_params=params(8),
        name="paired",
    )(own, twin)


def feature_kernel(first, total_hbm, one_hbm, two_hbm, *refs):
    total_out, weighted_out, weight_out, margin_ref, buffer, sems = refs[-6:]
    blocks, samples = total_out.shape[:2]
    words = samples // BITS

    def copies(block):
        lanes = pl.ds((first + block) * LANES, LANES)
        return [
            pltpu.make_async_copy(ref.at[:, lanes], buffer.at[spot, block], sems.at[spot, block])
            for spot, ref in enumerate((total_hbm, one_hbm, two_hbm))
        ]

    for block in range(blocks):
        for copy in copies(block):
            copy.start()
    for block in range(blocks):
        for copy in copies(block):
            copy.wait()

        def step(bit, sums, block=block):
            log_sum, log_sq = sums
            for half in range(2):
                rows = pl.ds(bit + half * HALF, words, stride=BITS)
                spot = pl.ds(pl.multiple_of((2 * bit + half) * words, words), words)
                log_total = jnp.log(buffer[0, block, rows, :].astype(jnp.float32) + 1.0)
                one_plus = buffer[1, block, rows, :].astype(jnp.float32) + 1.0
                two_plus = buffer[2, block, rows, :].astype(jnp.float32) + 1.0
                log_ratio = jnp.log(one_plus / two_plus)
                weight = (one_plus * two_plus) / (one_plus + two_plus)
                total_out[block, spot, :] = log_total.astype(jnp.bfloat16)
                weighted_out[block, spot, :] = (weight * log_ratio).astype(jnp.bfloat16)
                weight_out[block, spot, :] = weight.astype(jnp.bfloat16)
                folded = log_total.reshape(words // 8, 8, LANES)
                log_sum = log_sum + jnp.sum(folded, axis=0)
                log_sq = log_sq + jnp.sum(folded * folded, axis=0)
            return log_sum, log_sq

        blank = jnp.zeros((8, LANES), jnp.float32)
        sums = lax.fori_loop(0, HALF, step, (blank, blank), unroll=3)
        for kind in range(2):
            margin_ref[kind : kind + 1, block * LANES : (block + 1) * LANES] = jnp.sum(
                sums[kind], axis=0, keepdims=True
            )


def features(total_counts, allele_one, allele_two, first, blocks, after):
    samples = total_counts.shape[0]
    width = blocks * LANES
    feature = jax.ShapeDtypeStruct((blocks, samples, LANES), jnp.bfloat16)
    return pl.pallas_call(
        functools.partial(feature_kernel, first),
        out_shape=(feature,) * 3 + (jax.ShapeDtypeStruct((2, width), jnp.float32),),
        in_specs=[pl.BlockSpec(memory_space=pltpu.HBM)] * 3
        + [pl.BlockSpec(memory_space=pl.ANY)] * len(after),
        out_specs=tuple(whole(4)),
        scratch_shapes=[
            pltpu.VMEM((3, blocks, samples, LANES), jnp.int32),
            pltpu.SemaphoreType.DMA((3, blocks)),
        ],
        cost_estimate=pl.CostEstimate(
            flops=12_000_000 * width, bytes_accessed=18 * samples * width, transcendentals=0
        ),
        compiler_params=params(44),
        name="features",
    )(total_counts, allele_one, allele_two, *after)


def cross_kernel(spots, part, margins, design_ref, *refs):
    keep_ref, send_ref = refs[-2:]
    calls = 1 + max(call for call, _ in spots)
    feature_refs, margin_refs = refs[:calls], refs[calls : calls + margins]
    half = design_ref.shape[0] // 2
    kept = half // 2
    for pair in range(len(spots) // 2):
        right = jnp.concatenate(
            [feature_refs[call][block] for call, block in spots[2 * pair : 2 * pair + 2]], axis=1
        )
        lanes = slice(pair * 2 * LANES, (pair + 1) * 2 * LANES)
        product = jnp.dot(
            design_ref[part * half : (part + 1) * half, :],
            right,
            preferred_element_type=jnp.float32,
        )
        keep_ref[:kept, lanes] = product[:kept]
        send_ref[:kept, lanes] = product[kept:]
    if margins:
        blank = jnp.zeros((EXTRA - 2, LANES), jnp.float32)
        for place, (call, block) in enumerate(spots):
            gene = margin_refs[call][:, block * LANES : (block + 1) * LANES]
            rest = blank
            if margins > calls:
                dos_ref = margin_refs[calls]
                picked = [
                    dos_ref[spot // 2, spot % 2 : spot % 2 + 1, :]
                    for spot in range(place, 2 * dos_ref.shape[0], len(spots))
                ]
                rest = jnp.concatenate([*picked, blank[len(picked) :]], axis=0)
            rows = jnp.concatenate([gene, rest], axis=0)
            lanes = slice(place * LANES, (place + 1) * LANES)
            keep_ref[kept:, lanes] = rows
            send_ref[kept:, lanes] = rows


def cross(design, features_of, spots, part, margins):
    variants, samples = design.shape
    width = len(spots) * LANES
    rows = variants // 4 + (EXTRA if margins else 0)
    out = jax.ShapeDtypeStruct((rows, width), jnp.float32)
    return pl.pallas_call(
        functools.partial(cross_kernel, spots, part, len(margins)),
        out_shape=(out, out),
        in_specs=whole(1 + len(features_of) + len(margins)),
        cost_estimate=pl.CostEstimate(
            flops=variants * samples * width,
            bytes_accessed=2 * (variants + width) * samples,
            transcendentals=0,
        ),
        compiler_params=params(8),
        name="cross",
    )(design, *features_of, *margins)


def meet_kernel(left_ref, right_ref, out_ref):
    out_ref[...] = left_ref[...] + right_ref[...]


def meet(left, right):
    return pl.pallas_call(
        meet_kernel,
        out_shape=jax.ShapeDtypeStruct(left.shape, left.dtype),
        in_specs=whole(2),
        compiler_params=params(8),
        name="meet",
    )(left, right)


def fold_kernel(turned, count, *refs):
    keep_ref, send_ref = refs[-2:]
    terms, margins = refs[:count], refs[count:-2]
    half = min(term.shape[0] for term in terms) // 2 // 64 * 64
    quarter = half // 2
    if turned:
        keep_spots = ((0, quarter), (2 * quarter, quarter))
        send_spots = ((quarter, quarter), (3 * quarter, quarter))
    else:
        keep_spots, send_spots = ((0, half),), ((half, half),)
    for out_ref, spots in ((send_ref, send_spots), (keep_ref, keep_spots)):
        at = 0
        for first, rows in spots:
            total = terms[0][first : first + rows]
            for term in terms[1:]:
                total = total + term[first : first + rows]
            out_ref[at : at + rows] = total
            at += rows
        if margins:
            start = margins[0].shape[0] - EXTRA
            total = margins[0][start:]
            for margin in margins[1:]:
                total = total + margin[margin.shape[0] - EXTRA :]
            out_ref[half:] = total


def fold(terms, margins, turned):
    rows, width = min(term.shape for term in terms)
    half = rows // 2 // 64 * 64
    out = jax.ShapeDtypeStruct((half + (EXTRA if margins else 0), width), jnp.float32)
    return pl.pallas_call(
        functools.partial(fold_kernel, turned, len(terms)),
        out_shape=(out, out),
        in_specs=whole(len(terms) + len(margins)),
        compiler_params=params(8),
        name="fold",
    )(*terms, *margins)


def finish_kernel(sample_count, where_ref, *refs):
    total_ref, allelic_ref = refs[-2:]
    own = total_ref.shape[0]
    samp = where_ref[0]
    chunks = len(CHUNKS)
    couples = [refs[at : at + 2] for at in range(0, 6 * chunks, 2)]
    pair_of = [couples[index * chunks : (index + 1) * chunks] for index in range(3)]
    margins = [left[own:, :] + right[own:, :] for left, right in pair_of[0]]
    columns = []
    for kind in range(2):
        picked = jnp.zeros((1, LANES), jnp.float32)
        for source in range(lax.axis_size("var")):
            spot = 2 * source + kind
            row, block = 2 + spot // CHUNKS[DOS_CHUNK], spot % CHUNKS[DOS_CHUNK]
            row_now = margins[DOS_CHUNK][row : row + 1, block * LANES : (block + 1) * LANES]
            picked = jnp.where(samp >> 1 == source, row_now, picked)
        turned = jnp.broadcast_to(picked, (LANES, LANES)).T
        columns.append(jnp.where(samp & 1 == 0, turned[:own], turned[own:]))
    dos_sum, dos_sq = columns
    dosage_var = dos_sq - dos_sum * dos_sum / sample_count
    scale = jnp.sqrt(jnp.float32(sample_count))
    first = 0
    for chunk, blocks in enumerate(CHUNKS):
        for block in range(blocks):
            lanes = slice(block * LANES, (block + 1) * LANES)
            spot = slice((first + block) * LANES, (first + block + 1) * LANES)
            gene_sum, gene_sq = margins[chunk][0:1, lanes], margins[chunk][1:2, lanes]
            gene_var = gene_sq - gene_sum * gene_sum / sample_count
            pair_sums = [
                pair_of[index][chunk][0][:own, lanes] + pair_of[index][chunk][1][:own, lanes]
                for index in range(3)
            ]
            covariance = pair_sums[0] - dos_sum * gene_sum / sample_count
            total_ref[:, spot] = (
                scale * covariance / jnp.sqrt((dosage_var + 1.0) * (gene_var + 1.0))
            )
            allelic_ref[:, spot] = pair_sums[1] / jnp.sqrt(pair_sums[2] + 1.0)
        first += blocks


def finish(where, parts, own, width, sample_count):
    out = jax.ShapeDtypeStruct((own, width), jnp.float32)
    return pl.pallas_call(
        functools.partial(finish_kernel, sample_count),
        out_shape=(out, out),
        in_specs=[pl.BlockSpec(memory_space=pltpu.SMEM)] + whole(len(parts)),
        compiler_params=params(8),
        name="finish",
    )(where, *parts)


def per_device(hap_words, total_counts, allele_one, allele_two):
    where = jnp.stack([lax.axis_index("samp"), lax.axis_index("var")]).astype(jnp.int32)
    twin = swap(hap_words, "var", 1)
    counts = (total_counts, allele_one, allele_two)
    made = []
    for call, blocks in enumerate(MADE):
        after = (twin,) if call else ()
        made.append(features(*counts, sum(MADE[:call]), blocks, after))
    pairs = [paired(hap_words, twin)]
    for flip in FAR:
        pairs.append(swap(pairs[0], "var", flip))
    *designs, dos_part = unpack(where, pairs)
    spots = [(call, block) for call, blocks in enumerate(MADE) for block in range(blocks)]
    kept, cored, sent, came = {}, {}, {}, {}
    for part, chunk, index in items():
        first = sum(CHUNKS[:chunk])
        mine = spots[first : first + CHUNKS[chunk]]
        calls = 1 + max(call for call, _ in mine)
        margins = []
        if index == 0 and part == 1:
            margins = [made[call][3] for call in range(calls)]
            margins += [dos_part] if chunk == DOS_CHUNK else []
        features_of = [made[call][index] for call in range(calls)]
        keep, send = cross(designs[index], features_of, mine, part, margins)
        got = swap(send, "samp", CORE)
        if part == 0:
            kept[chunk, index], cored[chunk, index] = keep, got
        else:
            sent[chunk, index] = meet(keep, got)
            came[chunk, index] = swap(sent[chunk, index], "samp", sides(index, chunk)[0])
    cells = [(chunk, index) for chunk in range(len(CHUNKS)) for index in range(3)]
    for chunk, index in cells:
        cell = chunk, index
        margins = [sent[cell], came[cell]] if index == 0 else []
        keep, send = fold(
            [kept[cell], cored[cell], came[cell]], margins, cell[::-1] in TURNED
        )
        kept[cell], came[cell] = keep, swap(send, "samp", sides(index, chunk)[1])
    for chunk, index in cells:
        cell = chunk, index
        margins = [kept[cell], came[cell]] if index == 0 else []
        keep, send = fold([kept[cell], came[cell]], margins, False)
        kept[cell], came[cell] = keep, swap(send, "samp", sides(index, chunk)[2])
    sample_count = float(total_counts.shape[0] * lax.axis_size("samp"))
    own = designs[0].shape[0] // lax.axis_size("samp")
    parts = []
    for index in range(3):
        for chunk in range(len(CHUNKS)):
            parts += [kept[chunk, index], came[chunk, index]]
    return finish(where, parts, own, total_counts.shape[1], sample_count)


def items():
    return [
        (part, chunk, index)
        for part in (1, 0)
        for chunk in range(len(CHUNKS))
        for index in range(3)
    ]


def solution(mesh):
    in_specs = (P(None, "samp", "var"), P("samp", "var"), P("samp", "var"), P("samp", "var"))
    out_specs = (P("samp", "var"), P("samp", "var"))

    return jax.shard_map(
        per_device, mesh=mesh, in_specs=in_specs, out_specs=out_specs, check_vma=False
    )
```

```python
import functools

import jax
import jax.numpy as jnp
from jax import lax
from jax.experimental import pallas as pl
from jax.experimental.pallas import tpu as pltpu
from jax.sharding import PartitionSpec as P

BITS = 30
HALF = BITS // 2
LANES = 128
MIB = 1024 * 1024
MADE = (2, 6)
CHUNKS = (4, 4)
DOS_CHUNK = 0
EXTRA = 8

CORE, SIDE_Y, SIDE_A, SIDE_B = 1, 2, 4, 12
ORDERS = ((SIDE_Y, SIDE_A, SIDE_B), (SIDE_A, SIDE_B, SIDE_Y), (SIDE_B, SIDE_Y, SIDE_A))
TURNED = ()
SENDING, KEEPING, FIRST, SECOND, THIRD = "sending", "keeping", "first", "second", "third"
PLAN = (
    (SENDING, 1, 1),
    (SENDING, 0, 0),
    (SENDING, 2, 0),
    (FIRST, 1, 1),
    (FIRST, 0, 0),
    (FIRST, 2, 0),
    (SENDING, 1, 0),
    (SENDING, 0, 1),
    (SENDING, 2, 1),
    (FIRST, 1, 0),
    (FIRST, 0, 1),
    (KEEPING, 1, 0),
    (FIRST, 2, 1),
    (KEEPING, 0, 0),
    (KEEPING, 1, 1),
    (KEEPING, 0, 1),
    (KEEPING, 2, 0),
    (SECOND, 0, 0),
    (SECOND, 1, 1),
    (SECOND, 2, 0),
    (KEEPING, 2, 1),
    (SECOND, 0, 1),
    (SECOND, 2, 1),
    (SECOND, 1, 0),
    (THIRD, 0, 0),
    (THIRD, 1, 1),
    (THIRD, 2, 0),
    (THIRD, 0, 1),
    (THIRD, 2, 1),
    (THIRD, 1, 0),
)
FAR = (4, 2, 6)


def swap(array, axis, flip):
    size = lax.axis_size(axis)
    return lax.ppermute(array, axis, [(d, d ^ flip) for d in range(size)])


def place_of(relative, order):
    bits = {
        SIDE_Y: (relative >> 1) & 1,
        SIDE_A: ((relative >> 2) ^ (relative >> 3)) & 1,
        SIDE_B: (relative >> 3) & 1,
    }
    first, second, third = order
    return 8 * bits[first] + 4 * (relative & 1) + 2 * bits[second] + bits[third]


def sides(index, chunk):
    first, second, third = ORDERS[index]
    return (first, third, second) if (index, chunk) in TURNED else (first, second, third)


def whole(count):
    return [pl.BlockSpec(memory_space=pltpu.VMEM)] * count


def params(mib):
    return pltpu.CompilerParams(vmem_limit_bytes=mib * MIB)


def unpack_kernel(where_ref, *refs):
    word_refs, (dosage_ref, phase_ref, mixed_ref, margin_ref) = refs[:-4], refs[-4:]
    samp, var = where_ref[0], where_ref[1]
    low = (1 << HALF) - 1
    words, block = word_refs[0].shape[1:]
    rows = block // 2
    samples = float(words * BITS)
    one, zero = jnp.bfloat16(1), jnp.bfloat16(0)
    pieces = [
        (flip + twin, word_ref, 2 * twin)
        for flip, word_ref in zip((0, *FAR), word_refs)
        for twin in range(2)
    ]
    for flip, word_ref, spot in pieces:
        source = var ^ flip
        first, second = word_ref[spot], word_ref[spot + 1]
        ones = lax.population_count(first) + lax.population_count(second)
        mixed = lax.population_count(first ^ second)
        margin_ref[pl.ds(source, 1), 0:1, :] = (
            jnp.sum(ones.astype(jnp.float32), axis=0, keepdims=True) - samples
        )[None]
        margin_ref[pl.ds(source, 1), 1:2, :] = (
            samples - jnp.sum(mixed.astype(jnp.float32), axis=0, keepdims=True)
        )[None]
        turned = [
            jnp.concatenate([w & low, (w >> HALF) & low], axis=0).T.astype(jnp.int16)
            for w in (first, second)
        ]
        for part in range(2):
            relative = (2 * source + part) ^ samp
            starts = [pl.multiple_of(place_of(relative, order) * rows, rows) for order in ORDERS]
            mine = [t[part * rows : (part + 1) * rows] for t in turned]
            for bit in range(HALF):
                mask = jnp.int16(1 << bit)
                hap_one = jnp.where((mine[0] & mask) != 0, one, zero)
                hap_two = jnp.where((mine[1] & mask) != 0, one, zero)
                phase = hap_one - hap_two
                lanes = slice(bit * 2 * words, (bit + 1) * 2 * words)
                dosage_ref[pl.ds(starts[0], rows), lanes] = (hap_one + hap_two) - one
                phase_ref[pl.ds(starts[1], rows), lanes] = phase
                mixed_ref[pl.ds(starts[2], rows), lanes] = phase * phase


def unpack(where, pairs):
    _, words, block = pairs[0].shape
    count = 2 * len(pairs)
    variants, samples = count * block, words * BITS
    design = jax.ShapeDtypeStruct((variants, samples), jnp.bfloat16)
    return pl.pallas_call(
        unpack_kernel,
        out_shape=(design,) * 3 + (jax.ShapeDtypeStruct((count, 2, block), jnp.float32),),
        in_specs=[pl.BlockSpec(memory_space=pltpu.SMEM)] + whole(len(pairs)),
        cost_estimate=pl.CostEstimate(
            flops=6_000_000_000, bytes_accessed=6 * variants * samples, transcendentals=0
        ),
        compiler_params=params(8),
        name="unpack",
    )(where, *pairs)


def pair_kernel(own_ref, twin_ref, pair_ref):
    pair_ref[:2] = own_ref[...]
    pair_ref[2:] = twin_ref[...]


def paired(own, twin):
    _, words, block = own.shape
    return pl.pallas_call(
        pair_kernel,
        out_shape=jax.ShapeDtypeStruct((4, words, block), own.dtype),
        in_specs=whole(2),
        compiler_params=params(8),
        name="paired",
    )(own, twin)


def feature_kernel(first, total_hbm, one_hbm, two_hbm, *refs):
    total_out, weighted_out, weight_out, margin_ref, buffer, sems = refs[-6:]
    blocks, samples = total_out.shape[:2]
    words = samples // BITS

    def copies(block):
        lanes = pl.ds((first + block) * LANES, LANES)
        return [
            pltpu.make_async_copy(ref.at[:, lanes], buffer.at[spot, block], sems.at[spot, block])
            for spot, ref in enumerate((total_hbm, one_hbm, two_hbm))
        ]

    for block in range(blocks):
        for copy in copies(block):
            copy.start()
    for block in range(blocks):
        for copy in copies(block):
            copy.wait()

        def step(bit, sums, block=block):
            log_sum, log_sq = sums
            for half in range(2):
                rows = pl.ds(bit + half * HALF, words, stride=BITS)
                spot = pl.ds(pl.multiple_of((2 * bit + half) * words, words), words)
                log_total = jnp.log(buffer[0, block, rows, :].astype(jnp.float32) + 1.0)
                one_plus = buffer[1, block, rows, :].astype(jnp.float32) + 1.0
                two_plus = buffer[2, block, rows, :].astype(jnp.float32) + 1.0
                log_ratio = jnp.log(one_plus / two_plus)
                weight = (one_plus * two_plus) / (one_plus + two_plus)
                total_out[block, spot, :] = log_total.astype(jnp.bfloat16)
                weighted_out[block, spot, :] = (weight * log_ratio).astype(jnp.bfloat16)
                weight_out[block, spot, :] = weight.astype(jnp.bfloat16)
                folded = log_total.reshape(words // 8, 8, LANES)
                log_sum = log_sum + jnp.sum(folded, axis=0)
                log_sq = log_sq + jnp.sum(folded * folded, axis=0)
            return log_sum, log_sq

        blank = jnp.zeros((8, LANES), jnp.float32)
        sums = lax.fori_loop(0, HALF, step, (blank, blank), unroll=3)
        for kind in range(2):
            margin_ref[kind : kind + 1, block * LANES : (block + 1) * LANES] = jnp.sum(
                sums[kind], axis=0, keepdims=True
            )


def features(total_counts, allele_one, allele_two, first, blocks, after):
    samples = total_counts.shape[0]
    width = blocks * LANES
    feature = jax.ShapeDtypeStruct((blocks, samples, LANES), jnp.bfloat16)
    return pl.pallas_call(
        functools.partial(feature_kernel, first),
        out_shape=(feature,) * 3 + (jax.ShapeDtypeStruct((2, width), jnp.float32),),
        in_specs=[pl.BlockSpec(memory_space=pltpu.HBM)] * 3
        + [pl.BlockSpec(memory_space=pl.ANY)] * len(after),
        out_specs=tuple(whole(4)),
        scratch_shapes=[
            pltpu.VMEM((3, blocks, samples, LANES), jnp.int32),
            pltpu.SemaphoreType.DMA((3, blocks)),
        ],
        cost_estimate=pl.CostEstimate(
            flops=12_000_000 * width, bytes_accessed=18 * samples * width, transcendentals=0
        ),
        compiler_params=params(44),
        name="features",
    )(total_counts, allele_one, allele_two, *after)


def cross_kernel(spots, part, margins, design_ref, *refs):
    keep_ref, send_ref = refs[-2:]
    calls = 1 + max(call for call, _ in spots)
    feature_refs, margin_refs = refs[:calls], refs[calls : calls + margins]
    half = design_ref.shape[0] // 2
    kept = half // 2
    for pair in range(len(spots) // 2):
        right = jnp.concatenate(
            [feature_refs[call][block] for call, block in spots[2 * pair : 2 * pair + 2]], axis=1
        )
        lanes = slice(pair * 2 * LANES, (pair + 1) * 2 * LANES)
        product = jnp.dot(
            design_ref[part * half : (part + 1) * half, :],
            right,
            preferred_element_type=jnp.float32,
        )
        keep_ref[:kept, lanes] = product[:kept]
        send_ref[:kept, lanes] = product[kept:]
    if margins:
        blank = jnp.zeros((EXTRA - 2, LANES), jnp.float32)
        for place, (call, block) in enumerate(spots):
            gene = margin_refs[call][:, block * LANES : (block + 1) * LANES]
            rest = blank
            if margins > calls:
                dos_ref = margin_refs[calls]
                picked = [
                    dos_ref[spot // 2, spot % 2 : spot % 2 + 1, :]
                    for spot in range(place, 2 * dos_ref.shape[0], len(spots))
                ]
                rest = jnp.concatenate([*picked, blank[len(picked) :]], axis=0)
            rows = jnp.concatenate([gene, rest], axis=0)
            lanes = slice(place * LANES, (place + 1) * LANES)
            keep_ref[kept:, lanes] = rows
            send_ref[kept:, lanes] = rows


def cross(design, features_of, spots, part, margins):
    variants, samples = design.shape
    width = len(spots) * LANES
    rows = variants // 4 + (EXTRA if margins else 0)
    out = jax.ShapeDtypeStruct((rows, width), jnp.float32)
    return pl.pallas_call(
        functools.partial(cross_kernel, spots, part, len(margins)),
        out_shape=(out, out),
        in_specs=whole(1 + len(features_of) + len(margins)),
        cost_estimate=pl.CostEstimate(
            flops=variants * samples * width,
            bytes_accessed=2 * (variants + width) * samples,
            transcendentals=0,
        ),
        compiler_params=params(8),
        name="cross",
    )(design, *features_of, *margins)


def meet_kernel(left_ref, right_ref, out_ref):
    out_ref[...] = left_ref[...] + right_ref[...]


def meet(left, right):
    return pl.pallas_call(
        meet_kernel,
        out_shape=jax.ShapeDtypeStruct(left.shape, left.dtype),
        in_specs=whole(2),
        compiler_params=params(8),
        name="meet",
    )(left, right)


def fold_kernel(turned, count, *refs):
    keep_ref, send_ref = refs[-2:]
    terms, margins = refs[:count], refs[count:-2]
    half = min(term.shape[0] for term in terms) // 2 // 64 * 64
    quarter = half // 2
    if turned:
        keep_spots = ((0, quarter), (2 * quarter, quarter))
        send_spots = ((quarter, quarter), (3 * quarter, quarter))
    else:
        keep_spots, send_spots = ((0, half),), ((half, half),)
    for out_ref, spots in ((send_ref, send_spots), (keep_ref, keep_spots)):
        at = 0
        for first, rows in spots:
            total = terms[0][first : first + rows]
            for term in terms[1:]:
                total = total + term[first : first + rows]
            out_ref[at : at + rows] = total
            at += rows
        if margins:
            start = margins[0].shape[0] - EXTRA
            total = margins[0][start:]
            for margin in margins[1:]:
                total = total + margin[margin.shape[0] - EXTRA :]
            out_ref[half:] = total


def fold(terms, margins, turned):
    rows, width = min(term.shape for term in terms)
    half = rows // 2 // 64 * 64
    out = jax.ShapeDtypeStruct((half + (EXTRA if margins else 0), width), jnp.float32)
    return pl.pallas_call(
        functools.partial(fold_kernel, turned, len(terms)),
        out_shape=(out, out),
        in_specs=whole(len(terms) + len(margins)),
        compiler_params=params(8),
        name="fold",
    )(*terms, *margins)


def finish_kernel(sample_count, where_ref, *refs):
    total_ref, allelic_ref = refs[-2:]
    own = total_ref.shape[0]
    samp = where_ref[0]
    chunks = len(CHUNKS)
    couples = [refs[at : at + 2] for at in range(0, 6 * chunks, 2)]
    pair_of = [couples[index * chunks : (index + 1) * chunks] for index in range(3)]
    margins = [left[own:, :] + right[own:, :] for left, right in pair_of[0]]
    columns = []
    for kind in range(2):
        picked = jnp.zeros((1, LANES), jnp.float32)
        for source in range(lax.axis_size("var")):
            spot = 2 * source + kind
            row, block = 2 + spot // CHUNKS[DOS_CHUNK], spot % CHUNKS[DOS_CHUNK]
            row_now = margins[DOS_CHUNK][row : row + 1, block * LANES : (block + 1) * LANES]
            picked = jnp.where(samp >> 1 == source, row_now, picked)
        turned = jnp.broadcast_to(picked, (LANES, LANES)).T
        columns.append(jnp.where(samp & 1 == 0, turned[:own], turned[own:]))
    dos_sum, dos_sq = columns
    dosage_var = dos_sq - dos_sum * dos_sum / sample_count
    scale = jnp.sqrt(jnp.float32(sample_count))
    first = 0
    for chunk, blocks in enumerate(CHUNKS):
        for block in range(blocks):
            lanes = slice(block * LANES, (block + 1) * LANES)
            spot = slice((first + block) * LANES, (first + block + 1) * LANES)
            gene_sum, gene_sq = margins[chunk][0:1, lanes], margins[chunk][1:2, lanes]
            gene_var = gene_sq - gene_sum * gene_sum / sample_count
            pair_sums = [
                pair_of[index][chunk][0][:own, lanes] + pair_of[index][chunk][1][:own, lanes]
                for index in range(3)
            ]
            covariance = pair_sums[0] - dos_sum * gene_sum / sample_count
            total_ref[:, spot] = (
                scale * covariance / jnp.sqrt((dosage_var + 1.0) * (gene_var + 1.0))
            )
            allelic_ref[:, spot] = pair_sums[1] / jnp.sqrt(pair_sums[2] + 1.0)
        first += blocks


def finish(where, parts, own, width, sample_count):
    out = jax.ShapeDtypeStruct((own, width), jnp.float32)
    return pl.pallas_call(
        functools.partial(finish_kernel, sample_count),
        out_shape=(out, out),
        in_specs=[pl.BlockSpec(memory_space=pltpu.SMEM)] + whole(len(parts)),
        compiler_params=params(8),
        name="finish",
    )(where, *parts)


def per_device(hap_words, total_counts, allele_one, allele_two):
    where = jnp.stack([lax.axis_index("samp"), lax.axis_index("var")]).astype(jnp.int32)
    twin = swap(hap_words, "var", 1)
    counts = (total_counts, allele_one, allele_two)
    made = []
    for call, blocks in enumerate(MADE):
        after = (twin,) if call else ()
        made.append(features(*counts, sum(MADE[:call]), blocks, after))
    pairs = [paired(hap_words, twin)]
    for flip in FAR:
        pairs.append(swap(pairs[0], "var", flip))
    *designs, dos_part = unpack(where, pairs)
    spots = [(call, block) for call, blocks in enumerate(MADE) for block in range(blocks)]
    kept, sent, came = {}, {}, {}
    for kind, index, chunk in PLAN:
        cell = index, chunk
        if kind in (SENDING, KEEPING):
            first = sum(CHUNKS[:chunk])
            mine = spots[first : first + CHUNKS[chunk]]
            calls = 1 + max(call for call, _ in mine)
            margins = []
            if index == 0 and kind == SENDING:
                margins = [made[call][3] for call in range(calls)]
                margins += [dos_part] if chunk == DOS_CHUNK else []
            features_of = [made[call][index] for call in range(calls)]
            part = int(kind == SENDING)
            keep, send = cross(designs[index], features_of, mine, part, margins)
        elif kind == FIRST:
            keep, send = None, meet(kept[SENDING, cell], came[SENDING, cell])
            sent[cell] = send
        elif kind == SECOND:
            terms = [kept[KEEPING, cell], came[KEEPING, cell], came[FIRST, cell]]
            margins = [sent[cell], came[FIRST, cell]] if index == 0 else []
            keep, send = fold(terms, margins, cell in TURNED)
        else:
            terms = [kept[SECOND, cell], came[SECOND, cell]]
            keep, send = fold(terms, terms if index == 0 else [], False)
        at = (FIRST, SECOND, THIRD).index(kind) if kind in (FIRST, SECOND, THIRD) else None
        side = CORE if at is None else sides(index, chunk)[at]
        kept[kind, cell], came[kind, cell] = keep, swap(send, "samp", side)
    sample_count = float(total_counts.shape[0] * lax.axis_size("samp"))
    own = designs[0].shape[0] // lax.axis_size("samp")
    parts = []
    for index in range(3):
        for chunk in range(len(CHUNKS)):
            parts += [kept[THIRD, (index, chunk)], came[THIRD, (index, chunk)]]
    return finish(where, parts, own, total_counts.shape[1], sample_count)


def solution(mesh):
    in_specs = (P(None, "samp", "var"), P("samp", "var"), P("samp", "var"), P("samp", "var"))
    out_specs = (P("samp", "var"), P("samp", "var"))

    return jax.shard_map(
        per_device, mesh=mesh, in_specs=in_specs, out_specs=out_specs, check_vma=False
    )
```

```python
import functools

import jax
import jax.numpy as jnp
from jax import lax
from jax.experimental import pallas as pl
from jax.experimental.pallas import tpu as pltpu
from jax.sharding import PartitionSpec as P

BITS = 30
HALF = BITS // 2
LANES = 128
MIB = 1024 * 1024
MADE = (2, 6)
CHUNKS = (4, 4)
RIDE = (0, 0)
EXTRA = 8

CORE, SIDE_Y, SIDE_A, SIDE_B = 1, 2, 4, 12
ORDERS = ((SIDE_Y, SIDE_A, SIDE_B), (SIDE_A, SIDE_B, SIDE_Y), (SIDE_B, SIDE_Y, SIDE_A))
TURNED = ()
SENDING, KEEPING, FIRST, SECOND, THIRD = "sending", "keeping", "first", "second", "third"
PLAN = (
    (SENDING, 1, 0),
    (SENDING, 0, 1),
    (SENDING, 2, 1),
    (FIRST, 1, 0),
    (FIRST, 0, 1),
    (FIRST, 2, 1),
    (SENDING, 1, 1),
    (SENDING, 0, 0),
    (SENDING, 2, 0),
    (FIRST, 1, 1),
    (FIRST, 2, 0),
    (FIRST, 0, 0),
    (KEEPING, 1, 0),
    (KEEPING, 2, 0),
    (KEEPING, 2, 1),
    (KEEPING, 0, 1),
    (SECOND, 2, 1),
    (SECOND, 0, 1),
    (SECOND, 1, 0),
    (KEEPING, 0, 0),
    (KEEPING, 1, 1),
    (SECOND, 0, 0),
    (SECOND, 2, 0),
    (SECOND, 1, 1),
    (THIRD, 2, 1),
    (THIRD, 1, 0),
    (THIRD, 0, 1),
    (THIRD, 0, 0),
    (THIRD, 2, 0),
    (THIRD, 1, 1),
)
FAR = (4, 2, 6)


def swap(array, axis, flip):
    size = lax.axis_size(axis)
    return lax.ppermute(array, axis, [(d, d ^ flip) for d in range(size)])


def place_of(relative, order):
    bits = {
        SIDE_Y: (relative >> 1) & 1,
        SIDE_A: ((relative >> 2) ^ (relative >> 3)) & 1,
        SIDE_B: (relative >> 3) & 1,
    }
    first, second, third = order
    return 8 * bits[first] + 4 * (relative & 1) + 2 * bits[second] + bits[third]


def sides(index, chunk):
    first, second, third = ORDERS[index]
    return (first, third, second) if (index, chunk) in TURNED else (first, second, third)


def whole(count):
    return [pl.BlockSpec(memory_space=pltpu.VMEM)] * count


def params(mib):
    return pltpu.CompilerParams(vmem_limit_bytes=mib * MIB)


def unpack_kernel(where_ref, *refs):
    word_refs, (dosage_ref, phase_ref, mixed_ref, margin_ref) = refs[:-4], refs[-4:]
    samp, var = where_ref[0], where_ref[1]
    low = (1 << HALF) - 1
    words, block = word_refs[0].shape[1:]
    rows = block // 2
    samples = float(words * BITS)
    one, zero = jnp.bfloat16(1), jnp.bfloat16(0)
    pieces = [
        (flip + twin, word_ref, 2 * twin)
        for flip, word_ref in zip((0, *FAR), word_refs)
        for twin in range(2)
    ]
    for flip, word_ref, spot in pieces:
        source = var ^ flip
        first, second = word_ref[spot], word_ref[spot + 1]
        ones = lax.population_count(first) + lax.population_count(second)
        mixed = lax.population_count(first ^ second)
        margin_ref[pl.ds(source, 1), 0:1, :] = (
            jnp.sum(ones.astype(jnp.float32), axis=0, keepdims=True) - samples
        )[None]
        margin_ref[pl.ds(source, 1), 1:2, :] = (
            samples - jnp.sum(mixed.astype(jnp.float32), axis=0, keepdims=True)
        )[None]
        turned = [
            jnp.concatenate([w & low, (w >> HALF) & low], axis=0).T.astype(jnp.int16)
            for w in (first, second)
        ]
        for part in range(2):
            relative = (2 * source + part) ^ samp
            starts = [pl.multiple_of(place_of(relative, order) * rows, rows) for order in ORDERS]
            mine = [t[part * rows : (part + 1) * rows] for t in turned]
            wide = [jnp.concatenate([m, m], axis=1) for m in mine]
            lane = lax.broadcasted_iota(jnp.int32, wide[0].shape, 1)
            for bit in range(0, HALF, 2):
                both = min(2, HALF - bit)
                used = wide if both == 2 else mine
                mask = jnp.int16(1 << bit)
                if both == 2:
                    mask = jnp.where(lane < 2 * words, 1 << bit, 2 << bit).astype(jnp.int16)
                hap_one = jnp.where((used[0] & mask) != 0, one, zero)
                hap_two = jnp.where((used[1] & mask) != 0, one, zero)
                phase = hap_one - hap_two
                lanes = slice(bit * 2 * words, (bit + both) * 2 * words)
                dosage_ref[pl.ds(starts[0], rows), lanes] = (hap_one + hap_two) - one
                phase_ref[pl.ds(starts[1], rows), lanes] = phase
                mixed_ref[pl.ds(starts[2], rows), lanes] = phase * phase


def unpack(where, pairs):
    _, words, block = pairs[0].shape
    count = 2 * len(pairs)
    variants, samples = count * block, words * BITS
    design = jax.ShapeDtypeStruct((variants, samples), jnp.bfloat16)
    return pl.pallas_call(
        unpack_kernel,
        out_shape=(design,) * 3 + (jax.ShapeDtypeStruct((count, 2, block), jnp.float32),),
        in_specs=[pl.BlockSpec(memory_space=pltpu.SMEM)] + whole(len(pairs)),
        cost_estimate=pl.CostEstimate(
            flops=6_000_000_000, bytes_accessed=6 * variants * samples, transcendentals=0
        ),
        compiler_params=params(8),
        name="unpack",
    )(where, *pairs)


def pair_kernel(own_ref, twin_ref, pair_ref):
    pair_ref[:2] = own_ref[...]
    pair_ref[2:] = twin_ref[...]


def paired(own, twin):
    _, words, block = own.shape
    return pl.pallas_call(
        pair_kernel,
        out_shape=jax.ShapeDtypeStruct((4, words, block), own.dtype),
        in_specs=whole(2),
        compiler_params=params(8),
        name="paired",
    )(own, twin)


def feature_kernel(first, total_hbm, one_hbm, two_hbm, *refs):
    total_out, weighted_out, weight_out, margin_ref, buffer, sems = refs[-6:]
    blocks, samples = total_out.shape[:2]
    words = samples // BITS

    def copies(block):
        lanes = pl.ds((first + block) * LANES, LANES)
        return [
            pltpu.make_async_copy(ref.at[:, lanes], buffer.at[spot, block], sems.at[spot, block])
            for spot, ref in enumerate((total_hbm, one_hbm, two_hbm))
        ]

    for block in range(blocks):
        for copy in copies(block):
            copy.start()
    for block in range(blocks):
        for copy in copies(block):
            copy.wait()

        def step(bit, sums, block=block):
            log_sum, log_sq = sums
            for half in range(2):
                rows = pl.ds(bit + half * HALF, words, stride=BITS)
                spot = pl.ds(pl.multiple_of((2 * bit + half) * words, words), words)
                log_total = jnp.log(buffer[0, block, rows, :].astype(jnp.float32) + 1.0)
                one_plus = buffer[1, block, rows, :].astype(jnp.float32) + 1.0
                two_plus = buffer[2, block, rows, :].astype(jnp.float32) + 1.0
                log_ratio = jnp.log(one_plus / two_plus)
                weight = (one_plus * two_plus) / (one_plus + two_plus)
                total_out[block, spot, :] = log_total.astype(jnp.bfloat16)
                weighted_out[block, spot, :] = (weight * log_ratio).astype(jnp.bfloat16)
                weight_out[block, spot, :] = weight.astype(jnp.bfloat16)
                folded = log_total.reshape(words // 8, 8, LANES)
                log_sum = log_sum + jnp.sum(folded, axis=0)
                log_sq = log_sq + jnp.sum(folded * folded, axis=0)
            return log_sum, log_sq

        blank = jnp.zeros((8, LANES), jnp.float32)
        sums = lax.fori_loop(0, HALF, step, (blank, blank), unroll=3)
        for kind in range(2):
            margin_ref[kind : kind + 1, block * LANES : (block + 1) * LANES] = jnp.sum(
                sums[kind], axis=0, keepdims=True
            )


def features(total_counts, allele_one, allele_two, first, blocks, after):
    samples = total_counts.shape[0]
    width = blocks * LANES
    feature = jax.ShapeDtypeStruct((blocks, samples, LANES), jnp.bfloat16)
    return pl.pallas_call(
        functools.partial(feature_kernel, first),
        out_shape=(feature,) * 3 + (jax.ShapeDtypeStruct((2, width), jnp.float32),),
        in_specs=[pl.BlockSpec(memory_space=pltpu.HBM)] * 3
        + [pl.BlockSpec(memory_space=pl.ANY)] * len(after),
        out_specs=tuple(whole(4)),
        scratch_shapes=[
            pltpu.VMEM((3, blocks, samples, LANES), jnp.int32),
            pltpu.SemaphoreType.DMA((3, blocks)),
        ],
        cost_estimate=pl.CostEstimate(
            flops=12_000_000 * width, bytes_accessed=18 * samples * width, transcendentals=0
        ),
        compiler_params=params(44),
        name="features",
    )(total_counts, allele_one, allele_two, *after)


def margin_rows(place, margin_refs):
    *gene_refs, dos_ref = margin_refs
    rows, first = [], 0
    for blocks in CHUNKS:
        call = 0
        at = first + place
        while at >= MADE[call]:
            at -= MADE[call]
            call += 1
        rows.append(gene_refs[call][:, at * LANES : (at + 1) * LANES])
        first += blocks
    stride = CHUNKS[RIDE[1]]
    for spot in range(place, 2 * dos_ref.shape[0], stride):
        rows.append(dos_ref[spot // 2, spot % 2 : spot % 2 + 1, :])
    return jnp.concatenate(rows, axis=0)


def cross_kernel(spots, part, margins, design_ref, *refs):
    keep_ref, send_ref = refs[-2:]
    calls = 1 + max(call for call, _ in spots)
    feature_refs, margin_refs = refs[:calls], refs[calls : calls + margins]
    half = design_ref.shape[0] // 2
    kept = half // 2
    for pair in range(len(spots) // 2):
        right = jnp.concatenate(
            [feature_refs[call][block] for call, block in spots[2 * pair : 2 * pair + 2]], axis=1
        )
        lanes = slice(pair * 2 * LANES, (pair + 1) * 2 * LANES)
        product = jnp.dot(
            design_ref[part * half : (part + 1) * half, :],
            right,
            preferred_element_type=jnp.float32,
        )
        keep_ref[:kept, lanes] = product[:kept]
        send_ref[:kept, lanes] = product[kept:]
    if margins:
        for place in range(len(spots)):
            rows = margin_rows(place, margin_refs)
            lanes = slice(place * LANES, (place + 1) * LANES)
            keep_ref[kept:, lanes] = rows
            send_ref[kept:, lanes] = rows


def cross(design, features_of, spots, part, margins):
    variants, samples = design.shape
    width = len(spots) * LANES
    rows = variants // 4 + (EXTRA if margins else 0)
    out = jax.ShapeDtypeStruct((rows, width), jnp.float32)
    return pl.pallas_call(
        functools.partial(cross_kernel, spots, part, len(margins)),
        out_shape=(out, out),
        in_specs=whole(1 + len(features_of) + len(margins)),
        cost_estimate=pl.CostEstimate(
            flops=variants * samples * width,
            bytes_accessed=2 * (variants + width) * samples,
            transcendentals=0,
        ),
        compiler_params=params(8),
        name="cross",
    )(design, *features_of, *margins)


def meet_kernel(left_ref, right_ref, out_ref):
    out_ref[...] = left_ref[...] + right_ref[...]


def meet(left, right):
    return pl.pallas_call(
        meet_kernel,
        out_shape=jax.ShapeDtypeStruct(left.shape, left.dtype),
        in_specs=whole(2),
        compiler_params=params(8),
        name="meet",
    )(left, right)


def fold_kernel(turned, count, *refs):
    keep_ref, send_ref = refs[-2:]
    terms, margins = refs[:count], refs[count:-2]
    half = min(term.shape[0] for term in terms) // 2 // 64 * 64
    quarter = half // 2
    if turned:
        keep_spots = ((0, quarter), (2 * quarter, quarter))
        send_spots = ((quarter, quarter), (3 * quarter, quarter))
    else:
        keep_spots, send_spots = ((0, half),), ((half, half),)
    for out_ref, spots in ((send_ref, send_spots), (keep_ref, keep_spots)):
        at = 0
        for first, rows in spots:
            total = terms[0][first : first + rows]
            for term in terms[1:]:
                total = total + term[first : first + rows]
            out_ref[at : at + rows] = total
            at += rows
        if margins:
            start = margins[0].shape[0] - EXTRA
            total = margins[0][start:]
            for margin in margins[1:]:
                total = total + margin[margin.shape[0] - EXTRA :]
            out_ref[half:] = total


def fold(terms, margins, turned):
    rows, width = min(term.shape for term in terms)
    half = rows // 2 // 64 * 64
    out = jax.ShapeDtypeStruct((half + (EXTRA if margins else 0), width), jnp.float32)
    return pl.pallas_call(
        functools.partial(fold_kernel, turned, len(terms)),
        out_shape=(out, out),
        in_specs=whole(len(terms) + len(margins)),
        compiler_params=params(8),
        name="fold",
    )(*terms, *margins)


def finish_kernel(sample_count, where_ref, *refs):
    total_hbm, allelic_hbm, total_ref, allelic_ref, sems = refs[-5:]
    own = total_ref.shape[0]
    samp = where_ref[0]
    chunks = len(CHUNKS)
    couples = [refs[at : at + 2] for at in range(0, 6 * chunks, 2)]
    pair_of = [couples[index * chunks : (index + 1) * chunks] for index in range(3)]
    left, right = pair_of[RIDE[0]][RIDE[1]]
    margin = left[own:, :] + right[own:, :]
    stride = CHUNKS[RIDE[1]]
    columns = []
    for kind in range(2):
        picked = jnp.zeros((1, LANES), jnp.float32)
        for source in range(lax.axis_size("var")):
            spot = 2 * source + kind
            row, block = 2 * chunks + spot // stride, spot % stride
            row_now = margin[row : row + 1, block * LANES : (block + 1) * LANES]
            picked = jnp.where(samp >> 1 == source, row_now, picked)
        turned = jnp.broadcast_to(picked, (LANES, LANES)).T
        columns.append(jnp.where(samp & 1 == 0, turned[:own], turned[own:]))
    dos_sum, dos_sq = columns
    dosage_var = dos_sq - dos_sum * dos_sum / sample_count
    scale = jnp.sqrt(jnp.float32(sample_count))
    first, copies = 0, []
    for chunk, blocks in enumerate(CHUNKS):
        for block in range(blocks):
            lanes = slice(block * LANES, (block + 1) * LANES)
            spot = slice((first + block) * LANES, (first + block + 1) * LANES)
            gene_sum = margin[2 * chunk : 2 * chunk + 1, lanes]
            gene_sq = margin[2 * chunk + 1 : 2 * chunk + 2, lanes]
            gene_var = gene_sq - gene_sum * gene_sum / sample_count
            pair_sums = [
                pair_of[index][chunk][0][:own, lanes] + pair_of[index][chunk][1][:own, lanes]
                for index in range(3)
            ]
            covariance = pair_sums[0] - dos_sum * gene_sum / sample_count
            total_ref[:, spot] = (
                scale * covariance / jnp.sqrt((dosage_var + 1.0) * (gene_var + 1.0))
            )
            allelic_ref[:, spot] = pair_sums[1] / jnp.sqrt(pair_sums[2] + 1.0)
        lanes = pl.ds(first * LANES, blocks * LANES)
        for which, (ref, hbm) in enumerate(((total_ref, total_hbm), (allelic_ref, allelic_hbm))):
            copy = pltpu.make_async_copy(ref.at[:, lanes], hbm.at[:, lanes], sems.at[which, chunk])
            copy.start()
            copies.append(copy)
        first += blocks
    for copy in copies:
        copy.wait()


def finish(where, parts, own, width, sample_count):
    out = jax.ShapeDtypeStruct((own, width), jnp.float32)
    return pl.pallas_call(
        functools.partial(finish_kernel, sample_count),
        out_shape=(out, out),
        in_specs=[pl.BlockSpec(memory_space=pltpu.SMEM)] + whole(len(parts)),
        out_specs=(pl.BlockSpec(memory_space=pl.ANY),) * 2,
        scratch_shapes=[
            pltpu.VMEM((own, width), jnp.float32),
            pltpu.VMEM((own, width), jnp.float32),
            pltpu.SemaphoreType.DMA((2, len(CHUNKS))),
        ],
        compiler_params=params(8),
        name="finish",
    )(where, *parts)


def per_device(hap_words, total_counts, allele_one, allele_two):
    where = jnp.stack([lax.axis_index("samp"), lax.axis_index("var")]).astype(jnp.int32)
    twin = swap(hap_words, "var", 1)
    counts = (total_counts, allele_one, allele_two)
    made = []
    for call, blocks in enumerate(MADE):
        after = (twin,) if call else ()
        made.append(features(*counts, sum(MADE[:call]), blocks, after))
    pairs = [paired(hap_words, twin)]
    for flip in FAR:
        pairs.append(swap(pairs[0], "var", flip))
    *designs, dos_part = unpack(where, pairs)
    spots = [(call, block) for call, blocks in enumerate(MADE) for block in range(blocks)]
    kept, sent, came = {}, {}, {}
    for kind, index, chunk in PLAN:
        cell = index, chunk
        if kind in (SENDING, KEEPING):
            first = sum(CHUNKS[:chunk])
            mine = spots[first : first + CHUNKS[chunk]]
            calls = 1 + max(call for call, _ in mine)
            margins = []
            if cell == RIDE and kind == SENDING:
                margins = [*(parts[3] for parts in made), dos_part]
            features_of = [made[call][index] for call in range(calls)]
            part = int(kind == SENDING)
            keep, send = cross(designs[index], features_of, mine, part, margins)
        elif kind == FIRST:
            keep, send = None, meet(kept[SENDING, cell], came[SENDING, cell])
            sent[cell] = send
        elif kind == SECOND:
            terms = [kept[KEEPING, cell], came[KEEPING, cell], came[FIRST, cell]]
            margins = [sent[cell], came[FIRST, cell]] if cell == RIDE else []
            keep, send = fold(terms, margins, cell in TURNED)
        else:
            terms = [kept[SECOND, cell], came[SECOND, cell]]
            keep, send = fold(terms, terms if cell == RIDE else [], False)
        at = (FIRST, SECOND, THIRD).index(kind) if kind in (FIRST, SECOND, THIRD) else None
        side = CORE if at is None else sides(index, chunk)[at]
        kept[kind, cell], came[kind, cell] = keep, swap(send, "samp", side)
    sample_count = float(total_counts.shape[0] * lax.axis_size("samp"))
    own = designs[0].shape[0] // lax.axis_size("samp")
    parts = []
    for index in range(3):
        for chunk in range(len(CHUNKS)):
            parts += [kept[THIRD, (index, chunk)], came[THIRD, (index, chunk)]]
    return finish(where, parts, own, total_counts.shape[1], sample_count)


def solution(mesh):
    in_specs = (P(None, "samp", "var"), P("samp", "var"), P("samp", "var"), P("samp", "var"))
    out_specs = (P("samp", "var"), P("samp", "var"))

    return jax.shard_map(
        per_device, mesh=mesh, in_specs=in_specs, out_specs=out_specs, check_vma=False
    )
```

```python
import functools

import jax
import jax.numpy as jnp
from jax import lax
from jax.experimental import pallas as pl
from jax.experimental.pallas import tpu as pltpu
from jax.sharding import PartitionSpec as P

BITS = 30
HALF = BITS // 2
LANES = 128
MIB = 1024 * 1024
MADE = (2, 6)
CHUNKS = (4, 4)
RIDE = (0, 0)
EXTRA = 8

CORE, SIDE_Y, SIDE_A, SIDE_B = 1, 2, 4, 12
ORDERS = ((SIDE_Y, SIDE_A, SIDE_B), (SIDE_A, SIDE_B, SIDE_Y), (SIDE_B, SIDE_Y, SIDE_A))
TURNED = ()
SENDING, KEEPING, FIRST, SECOND, THIRD = "sending", "keeping", "first", "second", "third"
PLAN = (
    (SENDING, 1, 0),
    (SENDING, 0, 0),
    (SENDING, 2, 1),
    (FIRST, 1, 0),
    (FIRST, 0, 0),
    (FIRST, 2, 1),
    (SENDING, 1, 1),
    (SENDING, 0, 1),
    (SENDING, 2, 0),
    (KEEPING, 2, 1),
    (FIRST, 1, 1),
    (FIRST, 0, 1),
    (FIRST, 2, 0),
    (KEEPING, 1, 0),
    (KEEPING, 0, 0),
    (KEEPING, 0, 1),
    (SECOND, 0, 0),
    (SECOND, 1, 0),
    (KEEPING, 2, 0),
    (SECOND, 2, 1),
    (KEEPING, 1, 1),
    (SECOND, 0, 1),
    (SECOND, 2, 0),
    (SECOND, 1, 1),
    (THIRD, 0, 0),
    (THIRD, 2, 1),
    (THIRD, 1, 0),
    (THIRD, 0, 1),
    (THIRD, 2, 0),
    (THIRD, 1, 1),
)
FAR = (4, 2, 6)


def swap(array, axis, flip):
    size = lax.axis_size(axis)
    return lax.ppermute(array, axis, [(d, d ^ flip) for d in range(size)])


def place_of(relative, order):
    bits = {
        SIDE_Y: (relative >> 1) & 1,
        SIDE_A: ((relative >> 2) ^ (relative >> 3)) & 1,
        SIDE_B: (relative >> 3) & 1,
    }
    first, second, third = order
    return 8 * bits[first] + 4 * (relative & 1) + 2 * bits[second] + bits[third]


def sides(index, chunk):
    first, second, third = ORDERS[index]
    return (first, third, second) if (index, chunk) in TURNED else (first, second, third)


def whole(count):
    return [pl.BlockSpec(memory_space=pltpu.VMEM)] * count


def params(mib):
    return pltpu.CompilerParams(vmem_limit_bytes=mib * MIB)


def unpack_kernel(where_ref, *refs):
    word_refs = refs[:-6]
    dosage_ref, phase_ref, mixed_ref, margin_ref, wide_ref, mask_ref = refs[-6:]
    samp, var = where_ref[0], where_ref[1]
    low = (1 << HALF) - 1
    words, block = word_refs[0].shape[1:]
    rows = block // 2
    samples = float(words * BITS)
    one, zero = jnp.bfloat16(1), jnp.bfloat16(0)
    lane = lax.broadcasted_iota(jnp.int32, mask_ref.shape[1:], 1)
    for step in range(mask_ref.shape[0]):
        bits = jnp.where(lane < 2 * words, 1 << (2 * step), 2 << (2 * step))
        mask_ref[step] = bits.astype(jnp.int16)
    pieces = [
        (flip + twin, word_ref, 2 * twin)
        for flip, word_ref in zip((0, *FAR), word_refs)
        for twin in range(2)
    ]
    for flip, word_ref, spot in pieces:
        source = var ^ flip
        first, second = word_ref[spot], word_ref[spot + 1]
        ones = lax.population_count(first) + lax.population_count(second)
        mixed = lax.population_count(first ^ second)
        margin_ref[pl.ds(source, 1), 0:1, :] = (
            jnp.sum(ones.astype(jnp.float32), axis=0, keepdims=True) - samples
        )[None]
        margin_ref[pl.ds(source, 1), 1:2, :] = (
            samples - jnp.sum(mixed.astype(jnp.float32), axis=0, keepdims=True)
        )[None]
        turned = [
            jnp.concatenate([w & low, (w >> HALF) & low], axis=0).T.astype(jnp.int16)
            for w in (first, second)
        ]
        for part in range(2):
            relative = (2 * source + part) ^ samp
            starts = [pl.multiple_of(place_of(relative, order) * rows, rows) for order in ORDERS]
            mine = [t[part * rows : (part + 1) * rows] for t in turned]
            for hap, m in enumerate(mine):
                wide_ref[hap] = jnp.concatenate([m, m], axis=1)
            for bit in range(0, HALF, 2):
                both = min(2, HALF - bit)
                used = slice(0, both * 2 * words)
                mask = mask_ref[bit // 2, :, used]
                hap_one = jnp.where((wide_ref[0, :, used] & mask) != 0, one, zero)
                hap_two = jnp.where((wide_ref[1, :, used] & mask) != 0, one, zero)
                phase = hap_one - hap_two
                lanes = slice(bit * 2 * words, (bit + both) * 2 * words)
                dosage_ref[pl.ds(starts[0], rows), lanes] = (hap_one + hap_two) - one
                phase_ref[pl.ds(starts[1], rows), lanes] = phase
                mixed_ref[pl.ds(starts[2], rows), lanes] = phase * phase


def unpack(where, pairs):
    _, words, block = pairs[0].shape
    count = 2 * len(pairs)
    variants, samples = count * block, words * BITS
    design = jax.ShapeDtypeStruct((variants, samples), jnp.bfloat16)
    return pl.pallas_call(
        unpack_kernel,
        out_shape=(design,) * 3 + (jax.ShapeDtypeStruct((count, 2, block), jnp.float32),),
        in_specs=[pl.BlockSpec(memory_space=pltpu.SMEM)] + whole(len(pairs)),
        scratch_shapes=[
            pltpu.VMEM((2, block // 2, 4 * words), jnp.int16),
            pltpu.VMEM(((HALF + 1) // 2, block // 2, 4 * words), jnp.int16),
        ],
        cost_estimate=pl.CostEstimate(
            flops=6_000_000_000, bytes_accessed=6 * variants * samples, transcendentals=0
        ),
        compiler_params=params(8),
        name="unpack",
    )(where, *pairs)


def pair_kernel(own_ref, twin_ref, pair_ref):
    pair_ref[:2] = own_ref[...]
    pair_ref[2:] = twin_ref[...]


def paired(own, twin):
    _, words, block = own.shape
    return pl.pallas_call(
        pair_kernel,
        out_shape=jax.ShapeDtypeStruct((4, words, block), own.dtype),
        in_specs=whole(2),
        compiler_params=params(8),
        name="paired",
    )(own, twin)


def feature_kernel(first, total_hbm, one_hbm, two_hbm, *refs):
    total_out, weighted_out, weight_out, margin_ref, buffer, sems = refs[-6:]
    blocks, samples = total_out.shape[:2]
    words = samples // BITS

    def copies(block):
        lanes = pl.ds((first + block) * LANES, LANES)
        return [
            pltpu.make_async_copy(ref.at[:, lanes], buffer.at[spot, block], sems.at[spot, block])
            for spot, ref in enumerate((total_hbm, one_hbm, two_hbm))
        ]

    for block in range(blocks):
        for copy in copies(block):
            copy.start()
    for block in range(blocks):
        for copy in copies(block):
            copy.wait()

        def step(bit, sums, block=block):
            log_sum, log_sq = sums
            for half in range(2):
                rows = pl.ds(bit + half * HALF, words, stride=BITS)
                spot = pl.ds(pl.multiple_of((2 * bit + half) * words, words), words)
                log_total = jnp.log(buffer[0, block, rows, :].astype(jnp.float32) + 1.0)
                one_plus = buffer[1, block, rows, :].astype(jnp.float32) + 1.0
                two_plus = buffer[2, block, rows, :].astype(jnp.float32) + 1.0
                log_ratio = jnp.log(one_plus / two_plus)
                weight = (one_plus * two_plus) / (one_plus + two_plus)
                total_out[block, spot, :] = log_total.astype(jnp.bfloat16)
                weighted_out[block, spot, :] = (weight * log_ratio).astype(jnp.bfloat16)
                weight_out[block, spot, :] = weight.astype(jnp.bfloat16)
                folded = log_total.reshape(words // 8, 8, LANES)
                log_sum = log_sum + jnp.sum(folded, axis=0)
                log_sq = log_sq + jnp.sum(folded * folded, axis=0)
            return log_sum, log_sq

        blank = jnp.zeros((8, LANES), jnp.float32)
        sums = lax.fori_loop(0, HALF, step, (blank, blank), unroll=3)
        for kind in range(2):
            margin_ref[kind : kind + 1, block * LANES : (block + 1) * LANES] = jnp.sum(
                sums[kind], axis=0, keepdims=True
            )


def features(total_counts, allele_one, allele_two, first, blocks, after):
    samples = total_counts.shape[0]
    width = blocks * LANES
    feature = jax.ShapeDtypeStruct((blocks, samples, LANES), jnp.bfloat16)
    return pl.pallas_call(
        functools.partial(feature_kernel, first),
        out_shape=(feature,) * 3 + (jax.ShapeDtypeStruct((2, width), jnp.float32),),
        in_specs=[pl.BlockSpec(memory_space=pltpu.HBM)] * 3
        + [pl.BlockSpec(memory_space=pl.ANY)] * len(after),
        out_specs=tuple(whole(4)),
        scratch_shapes=[
            pltpu.VMEM((3, blocks, samples, LANES), jnp.int32),
            pltpu.SemaphoreType.DMA((3, blocks)),
        ],
        cost_estimate=pl.CostEstimate(
            flops=12_000_000 * width, bytes_accessed=18 * samples * width, transcendentals=0
        ),
        compiler_params=params(44),
        name="features",
    )(total_counts, allele_one, allele_two, *after)


def margin_rows(place, margin_refs):
    *gene_refs, dos_ref = margin_refs
    rows, first = [], 0
    for blocks in CHUNKS:
        call = 0
        at = first + place
        while at >= MADE[call]:
            at -= MADE[call]
            call += 1
        rows.append(gene_refs[call][:, at * LANES : (at + 1) * LANES])
        first += blocks
    stride = CHUNKS[RIDE[1]]
    for spot in range(place, 2 * dos_ref.shape[0], stride):
        rows.append(dos_ref[spot // 2, spot % 2 : spot % 2 + 1, :])
    return jnp.concatenate(rows, axis=0)


def cross_kernel(spots, part, margins, design_ref, *refs):
    keep_ref, send_ref = refs[-2:]
    calls = 1 + max(call for call, _ in spots)
    feature_refs, margin_refs = refs[:calls], refs[calls : calls + margins]
    half = design_ref.shape[0] // 2
    kept = half // 2
    for pair in range(len(spots) // 2):
        right = jnp.concatenate(
            [feature_refs[call][block] for call, block in spots[2 * pair : 2 * pair + 2]], axis=1
        )
        lanes = slice(pair * 2 * LANES, (pair + 1) * 2 * LANES)
        product = jnp.dot(
            design_ref[part * half : (part + 1) * half, :],
            right,
            preferred_element_type=jnp.float32,
        )
        keep_ref[:kept, lanes] = product[:kept]
        send_ref[:kept, lanes] = product[kept:]
    if margins:
        for place in range(len(spots)):
            rows = margin_rows(place, margin_refs)
            lanes = slice(place * LANES, (place + 1) * LANES)
            keep_ref[kept:, lanes] = rows
            send_ref[kept:, lanes] = rows


def cross(design, features_of, spots, part, margins):
    variants, samples = design.shape
    width = len(spots) * LANES
    rows = variants // 4 + (EXTRA if margins else 0)
    out = jax.ShapeDtypeStruct((rows, width), jnp.float32)
    return pl.pallas_call(
        functools.partial(cross_kernel, spots, part, len(margins)),
        out_shape=(out, out),
        in_specs=whole(1 + len(features_of) + len(margins)),
        cost_estimate=pl.CostEstimate(
            flops=variants * samples * width,
            bytes_accessed=2 * (variants + width) * samples,
            transcendentals=0,
        ),
        compiler_params=params(8),
        name="cross",
    )(design, *features_of, *margins)


def meet_kernel(left_ref, right_ref, out_ref):
    out_ref[...] = left_ref[...] + right_ref[...]


def meet(left, right):
    return pl.pallas_call(
        meet_kernel,
        out_shape=jax.ShapeDtypeStruct(left.shape, left.dtype),
        in_specs=whole(2),
        compiler_params=params(8),
        name="meet",
    )(left, right)


def fold_kernel(turned, count, *refs):
    keep_ref, send_ref = refs[-2:]
    terms, margins = refs[:count], refs[count:-2]
    half = min(term.shape[0] for term in terms) // 2 // 64 * 64
    quarter = half // 2
    if turned:
        keep_spots = ((0, quarter), (2 * quarter, quarter))
        send_spots = ((quarter, quarter), (3 * quarter, quarter))
    else:
        keep_spots, send_spots = ((0, half),), ((half, half),)
    for out_ref, spots in ((send_ref, send_spots), (keep_ref, keep_spots)):
        at = 0
        for first, rows in spots:
            total = terms[0][first : first + rows]
            for term in terms[1:]:
                total = total + term[first : first + rows]
            out_ref[at : at + rows] = total
            at += rows
        if margins:
            start = margins[0].shape[0] - EXTRA
            total = margins[0][start:]
            for margin in margins[1:]:
                total = total + margin[margin.shape[0] - EXTRA :]
            out_ref[half:] = total


def fold(terms, margins, turned):
    rows, width = min(term.shape for term in terms)
    half = rows // 2 // 64 * 64
    out = jax.ShapeDtypeStruct((half + (EXTRA if margins else 0), width), jnp.float32)
    return pl.pallas_call(
        functools.partial(fold_kernel, turned, len(terms)),
        out_shape=(out, out),
        in_specs=whole(len(terms) + len(margins)),
        compiler_params=params(8),
        name="fold",
    )(*terms, *margins)


def finish_kernel(sample_count, where_ref, *refs):
    total_hbm, allelic_hbm, total_ref, allelic_ref, sems = refs[-5:]
    own = total_ref.shape[0]
    samp = where_ref[0]
    chunks = len(CHUNKS)
    couples = [refs[at : at + 2] for at in range(0, 6 * chunks, 2)]
    pair_of = [couples[index * chunks : (index + 1) * chunks] for index in range(3)]
    left, right = pair_of[RIDE[0]][RIDE[1]]
    margin = left[own:, :] + right[own:, :]
    stride = CHUNKS[RIDE[1]]
    columns = []
    for kind in range(2):
        picked = jnp.zeros((1, LANES), jnp.float32)
        for source in range(lax.axis_size("var")):
            spot = 2 * source + kind
            row, block = 2 * chunks + spot // stride, spot % stride
            row_now = margin[row : row + 1, block * LANES : (block + 1) * LANES]
            picked = jnp.where(samp >> 1 == source, row_now, picked)
        turned = jnp.broadcast_to(picked, (LANES, LANES)).T
        columns.append(jnp.where(samp & 1 == 0, turned[:own], turned[own:]))
    dos_sum, dos_sq = columns
    dosage_var = dos_sq - dos_sum * dos_sum / sample_count
    scale = jnp.sqrt(jnp.float32(sample_count))
    first, copies = 0, []
    for chunk, blocks in enumerate(CHUNKS):
        for block in range(blocks):
            lanes = slice(block * LANES, (block + 1) * LANES)
            spot = slice((first + block) * LANES, (first + block + 1) * LANES)
            gene_sum = margin[2 * chunk : 2 * chunk + 1, lanes]
            gene_sq = margin[2 * chunk + 1 : 2 * chunk + 2, lanes]
            gene_var = gene_sq - gene_sum * gene_sum / sample_count
            pair_sums = [
                pair_of[index][chunk][0][:own, lanes] + pair_of[index][chunk][1][:own, lanes]
                for index in range(3)
            ]
            covariance = pair_sums[0] - dos_sum * gene_sum / sample_count
            total_ref[:, spot] = (
                scale * covariance / jnp.sqrt((dosage_var + 1.0) * (gene_var + 1.0))
            )
            allelic_ref[:, spot] = pair_sums[1] / jnp.sqrt(pair_sums[2] + 1.0)
        lanes = pl.ds(first * LANES, blocks * LANES)
        for which, (ref, hbm) in enumerate(((total_ref, total_hbm), (allelic_ref, allelic_hbm))):
            copy = pltpu.make_async_copy(ref.at[:, lanes], hbm.at[:, lanes], sems.at[which, chunk])
            copy.start()
            copies.append(copy)
        first += blocks
    for copy in copies:
        copy.wait()


def finish(where, parts, own, width, sample_count):
    out = jax.ShapeDtypeStruct((own, width), jnp.float32)
    return pl.pallas_call(
        functools.partial(finish_kernel, sample_count),
        out_shape=(out, out),
        in_specs=[pl.BlockSpec(memory_space=pltpu.SMEM)] + whole(len(parts)),
        out_specs=(pl.BlockSpec(memory_space=pl.ANY),) * 2,
        scratch_shapes=[
            pltpu.VMEM((own, width), jnp.float32),
            pltpu.VMEM((own, width), jnp.float32),
            pltpu.SemaphoreType.DMA((2, len(CHUNKS))),
        ],
        compiler_params=params(8),
        name="finish",
    )(where, *parts)


def per_device(hap_words, total_counts, allele_one, allele_two):
    where = jnp.stack([lax.axis_index("samp"), lax.axis_index("var")]).astype(jnp.int32)
    twin = swap(hap_words, "var", 1)
    counts = (total_counts, allele_one, allele_two)
    made = []
    for call, blocks in enumerate(MADE):
        after = (twin,) if call else ()
        made.append(features(*counts, sum(MADE[:call]), blocks, after))
    pairs = [paired(hap_words, twin)]
    for flip in FAR:
        pairs.append(swap(pairs[0], "var", flip))
    *designs, dos_part = unpack(where, pairs)
    spots = [(call, block) for call, blocks in enumerate(MADE) for block in range(blocks)]
    kept, sent, came = {}, {}, {}
    for kind, index, chunk in PLAN:
        cell = index, chunk
        if kind in (SENDING, KEEPING):
            first = sum(CHUNKS[:chunk])
            mine = spots[first : first + CHUNKS[chunk]]
            calls = 1 + max(call for call, _ in mine)
            margins = []
            if cell == RIDE and kind == SENDING:
                margins = [*(parts[3] for parts in made), dos_part]
            features_of = [made[call][index] for call in range(calls)]
            part = int(kind == SENDING)
            keep, send = cross(designs[index], features_of, mine, part, margins)
        elif kind == FIRST:
            keep, send = None, meet(kept[SENDING, cell], came[SENDING, cell])
            sent[cell] = send
        elif kind == SECOND:
            terms = [kept[KEEPING, cell], came[KEEPING, cell], came[FIRST, cell]]
            margins = [sent[cell], came[FIRST, cell]] if cell == RIDE else []
            keep, send = fold(terms, margins, cell in TURNED)
        else:
            terms = [kept[SECOND, cell], came[SECOND, cell]]
            keep, send = fold(terms, terms if cell == RIDE else [], False)
        at = (FIRST, SECOND, THIRD).index(kind) if kind in (FIRST, SECOND, THIRD) else None
        side = CORE if at is None else sides(index, chunk)[at]
        kept[kind, cell], came[kind, cell] = keep, swap(send, "samp", side)
    sample_count = float(total_counts.shape[0] * lax.axis_size("samp"))
    own = designs[0].shape[0] // lax.axis_size("samp")
    parts = []
    for index in range(3):
        for chunk in range(len(CHUNKS)):
            parts += [kept[THIRD, (index, chunk)], came[THIRD, (index, chunk)]]
    return finish(where, parts, own, total_counts.shape[1], sample_count)


def solution(mesh):
    in_specs = (P(None, "samp", "var"), P("samp", "var"), P("samp", "var"), P("samp", "var"))
    out_specs = (P("samp", "var"), P("samp", "var"))

    return jax.shard_map(
        per_device, mesh=mesh, in_specs=in_specs, out_specs=out_specs, check_vma=False
    )
```

```python
import functools

import jax
import jax.numpy as jnp
from jax import lax
from jax.experimental import pallas as pl
from jax.experimental.pallas import tpu as pltpu
from jax.sharding import PartitionSpec as P

BITS = 30
HALF = BITS // 2
LANES = 128
MIB = 1024 * 1024
MADE = (2, 6)
CHUNKS = (4, 4)
RIDE = (0, 0)
EXTRA = 8

CORE, SIDE_Y, SIDE_A, SIDE_B = 1, 2, 4, 12
ORDERS = ((SIDE_Y, SIDE_A, SIDE_B), (SIDE_A, SIDE_B, SIDE_Y), (SIDE_B, SIDE_Y, SIDE_A))
TURNED = ()
SENDING, KEEPING, FIRST, SECOND, THIRD = "sending", "keeping", "first", "second", "third"
PLAN = (
    (SENDING, 1, 0),
    (SENDING, 0, 0),
    (SENDING, 2, 1),
    (FIRST, 1, 0),
    (FIRST, 0, 0),
    (FIRST, 2, 1),
    (SENDING, 1, 1),
    (SENDING, 0, 1),
    (SENDING, 2, 0),
    (KEEPING, 2, 1),
    (FIRST, 1, 1),
    (FIRST, 0, 1),
    (FIRST, 2, 0),
    (KEEPING, 1, 0),
    (KEEPING, 0, 0),
    (KEEPING, 0, 1),
    (SECOND, 0, 0),
    (SECOND, 1, 0),
    (KEEPING, 2, 0),
    (SECOND, 2, 1),
    (KEEPING, 1, 1),
    (SECOND, 0, 1),
    (SECOND, 2, 0),
    (SECOND, 1, 1),
    (THIRD, 0, 0),
    (THIRD, 2, 1),
    (THIRD, 1, 0),
    (THIRD, 0, 1),
    (THIRD, 2, 0),
    (THIRD, 1, 1),
)
FAR = (4, 2, 6)


def swap(array, axis, flip):
    size = lax.axis_size(axis)
    return lax.ppermute(array, axis, [(d, d ^ flip) for d in range(size)])


def place_of(relative, order):
    bits = {
        SIDE_Y: (relative >> 1) & 1,
        SIDE_A: ((relative >> 2) ^ (relative >> 3)) & 1,
        SIDE_B: (relative >> 3) & 1,
    }
    first, second, third = order
    return 8 * bits[first] + 4 * (relative & 1) + 2 * bits[second] + bits[third]


def sides(index, chunk):
    first, second, third = ORDERS[index]
    return (first, third, second) if (index, chunk) in TURNED else (first, second, third)


def whole(count):
    return [pl.BlockSpec(memory_space=pltpu.VMEM)] * count


def params(mib):
    return pltpu.CompilerParams(vmem_limit_bytes=mib * MIB)


def unpack_kernel(where_ref, *refs):
    word_refs = refs[:-6]
    dosage_ref, phase_ref, mixed_ref, margin_ref, wide_ref, mask_ref = refs[-6:]
    samp, var = where_ref[0], where_ref[1]
    low = (1 << HALF) - 1
    words, block = word_refs[0].shape[1:]
    rows = block // 2
    samples = float(words * BITS)
    one, zero = jnp.bfloat16(1), jnp.bfloat16(0)
    lane = lax.broadcasted_iota(jnp.int32, mask_ref.shape[1:], 1)
    for step in range(mask_ref.shape[0]):
        bits = jnp.where(lane < 2 * words, 1 << (2 * step), 2 << (2 * step))
        mask_ref[step] = bits.astype(jnp.int16)
    pieces = [
        (flip + twin, word_ref, 2 * twin)
        for flip, word_ref in zip((0, *FAR), word_refs)
        for twin in range(2)
    ]
    for flip, word_ref, spot in pieces:
        source = var ^ flip
        first, second = word_ref[spot], word_ref[spot + 1]
        ones = lax.population_count(first) + lax.population_count(second)
        mixed = lax.population_count(first ^ second)
        margin_ref[pl.ds(source, 1), 0:1, :] = (
            jnp.sum(ones.astype(jnp.float32), axis=0, keepdims=True) - samples
        )[None]
        margin_ref[pl.ds(source, 1), 1:2, :] = (
            samples - jnp.sum(mixed.astype(jnp.float32), axis=0, keepdims=True)
        )[None]
        turned = [
            jnp.concatenate([w & low, (w >> HALF) & low], axis=0).T.astype(jnp.int16)
            for w in (first, second)
        ]
        for part in range(2):
            relative = (2 * source + part) ^ samp
            starts = [pl.multiple_of(place_of(relative, order) * rows, rows) for order in ORDERS]
            mine = [t[part * rows : (part + 1) * rows] for t in turned]
            for hap, m in enumerate(mine):
                wide_ref[hap] = jnp.concatenate([m, m], axis=1)
            for bit in range(0, HALF, 2):
                both = min(2, HALF - bit)
                used = slice(0, both * 2 * words)
                mask = mask_ref[bit // 2, :, used]
                hap_one = jnp.where((wide_ref[0, :, used] & mask) != 0, one, zero)
                hap_two = jnp.where((wide_ref[1, :, used] & mask) != 0, one, zero)
                phase = hap_one - hap_two
                lanes = slice(bit * 2 * words, (bit + both) * 2 * words)
                dosage_ref[pl.ds(starts[0], rows), lanes] = (hap_one + hap_two) - one
                phase_ref[pl.ds(starts[1], rows), lanes] = phase
                mixed_ref[pl.ds(starts[2], rows), lanes] = phase * phase


def unpack(where, pairs):
    _, words, block = pairs[0].shape
    count = 2 * len(pairs)
    variants, samples = count * block, words * BITS
    design = jax.ShapeDtypeStruct((variants, samples), jnp.bfloat16)
    return pl.pallas_call(
        unpack_kernel,
        out_shape=(design,) * 3 + (jax.ShapeDtypeStruct((count, 2, block), jnp.float32),),
        in_specs=[pl.BlockSpec(memory_space=pltpu.SMEM)] + whole(len(pairs)),
        scratch_shapes=[
            pltpu.VMEM((2, block // 2, 4 * words), jnp.int16),
            pltpu.VMEM(((HALF + 1) // 2, block // 2, 4 * words), jnp.int16),
        ],
        cost_estimate=pl.CostEstimate(
            flops=6_000_000_000, bytes_accessed=6 * variants * samples, transcendentals=0
        ),
        compiler_params=params(8),
        name="unpack",
    )(where, *pairs)


def pair_kernel(own_ref, twin_ref, pair_ref):
    pair_ref[:2] = own_ref[...]
    pair_ref[2:] = twin_ref[...]


def paired(own, twin):
    _, words, block = own.shape
    return pl.pallas_call(
        pair_kernel,
        out_shape=jax.ShapeDtypeStruct((4, words, block), own.dtype),
        in_specs=whole(2),
        compiler_params=params(8),
        name="paired",
    )(own, twin)


def feature_kernel(first, total_hbm, one_hbm, two_hbm, *refs):
    total_out, weighted_out, weight_out, margin_ref, buffer, sems = refs[-6:]
    blocks, samples = total_out.shape[:2]
    words = samples // BITS

    def copies(block):
        lanes = pl.ds((first + block) * LANES, LANES)
        return [
            pltpu.make_async_copy(ref.at[:, lanes], buffer.at[spot, block], sems.at[spot, block])
            for spot, ref in enumerate((total_hbm, one_hbm, two_hbm))
        ]

    for block in range(blocks):
        for copy in copies(block):
            copy.start()
    for block in range(blocks):
        for copy in copies(block):
            copy.wait()

        def step(bit, sums, block=block):
            log_sum, log_sq = sums
            for half in range(2):
                rows = pl.ds(bit + half * HALF, words, stride=BITS)
                spot = pl.ds(pl.multiple_of((2 * bit + half) * words, words), words)
                log_total = jnp.log(buffer[0, block, rows, :].astype(jnp.float32) + 1.0)
                one_plus = buffer[1, block, rows, :].astype(jnp.float32) + 1.0
                two_plus = buffer[2, block, rows, :].astype(jnp.float32) + 1.0
                log_ratio = jnp.log(one_plus / two_plus)
                weight = (one_plus * two_plus) / (one_plus + two_plus)
                total_out[block, spot, :] = log_total.astype(jnp.bfloat16)
                weighted_out[block, spot, :] = (weight * log_ratio).astype(jnp.bfloat16)
                weight_out[block, spot, :] = weight.astype(jnp.bfloat16)
                folded = log_total.reshape(words // 8, 8, LANES)
                log_sum = log_sum + jnp.sum(folded, axis=0)
                log_sq = log_sq + jnp.sum(folded * folded, axis=0)
            return log_sum, log_sq

        blank = jnp.zeros((8, LANES), jnp.float32)
        sums = lax.fori_loop(0, HALF, step, (blank, blank), unroll=3)
        for kind in range(2):
            margin_ref[kind : kind + 1, block * LANES : (block + 1) * LANES] = jnp.sum(
                sums[kind], axis=0, keepdims=True
            )


def features(total_counts, allele_one, allele_two, first, blocks, after):
    samples = total_counts.shape[0]
    width = blocks * LANES
    feature = jax.ShapeDtypeStruct((blocks, samples, LANES), jnp.bfloat16)
    return pl.pallas_call(
        functools.partial(feature_kernel, first),
        out_shape=(feature,) * 3 + (jax.ShapeDtypeStruct((2, width), jnp.float32),),
        in_specs=[pl.BlockSpec(memory_space=pltpu.HBM)] * 3
        + [pl.BlockSpec(memory_space=pl.ANY)] * len(after),
        out_specs=tuple(whole(4)),
        scratch_shapes=[
            pltpu.VMEM((3, blocks, samples, LANES), jnp.int32),
            pltpu.SemaphoreType.DMA((3, blocks)),
        ],
        cost_estimate=pl.CostEstimate(
            flops=12_000_000 * width, bytes_accessed=18 * samples * width, transcendentals=0
        ),
        compiler_params=params(44),
        name="features",
    )(total_counts, allele_one, allele_two, *after)


def margin_rows(place, margin_refs):
    *gene_refs, dos_ref = margin_refs
    rows, first = [], 0
    for blocks in CHUNKS:
        call = 0
        at = first + place
        while at >= MADE[call]:
            at -= MADE[call]
            call += 1
        rows.append(gene_refs[call][:, at * LANES : (at + 1) * LANES])
        first += blocks
    stride = CHUNKS[RIDE[1]]
    for spot in range(place, 2 * dos_ref.shape[0], stride):
        rows.append(dos_ref[spot // 2, spot % 2 : spot % 2 + 1, :])
    return jnp.concatenate(rows, axis=0)


def cross_kernel(spots, part, margins, design_ref, *refs):
    keep_ref, send_ref = refs[-2:]
    calls = 1 + max(call for call, _ in spots)
    feature_refs, margin_refs = refs[:calls], refs[calls : calls + margins]
    half = design_ref.shape[0] // 2
    kept = half // 2
    for pair in range(len(spots) // 2):
        right = jnp.concatenate(
            [feature_refs[call][block] for call, block in spots[2 * pair : 2 * pair + 2]], axis=1
        )
        lanes = slice(pair * 2 * LANES, (pair + 1) * 2 * LANES)
        product = jnp.dot(
            design_ref[part * half : (part + 1) * half, :],
            right,
            preferred_element_type=jnp.float32,
        )
        keep_ref[:kept, lanes] = product[:kept]
        send_ref[:kept, lanes] = product[kept:]
    if margins:
        for place in range(len(spots)):
            rows = margin_rows(place, margin_refs)
            lanes = slice(place * LANES, (place + 1) * LANES)
            keep_ref[kept:, lanes] = rows
            send_ref[kept:, lanes] = rows


def cross(design, features_of, spots, part, margins):
    variants, samples = design.shape
    width = len(spots) * LANES
    rows = variants // 4 + (EXTRA if margins else 0)
    out = jax.ShapeDtypeStruct((rows, width), jnp.float32)
    return pl.pallas_call(
        functools.partial(cross_kernel, spots, part, len(margins)),
        out_shape=(out, out),
        in_specs=whole(1 + len(features_of) + len(margins)),
        cost_estimate=pl.CostEstimate(
            flops=variants * samples * width,
            bytes_accessed=2 * (variants + width) * samples,
            transcendentals=0,
        ),
        compiler_params=params(8),
        name="cross",
    )(design, *features_of, *margins)


def meet_kernel(left_ref, right_ref, out_ref):
    out_ref[...] = left_ref[...] + right_ref[...]


def meet(left, right):
    return pl.pallas_call(
        meet_kernel,
        out_shape=jax.ShapeDtypeStruct(left.shape, left.dtype),
        in_specs=whole(2),
        compiler_params=params(8),
        name="meet",
    )(left, right)


def fold_kernel(turned, count, *refs):
    keep_ref, send_ref = refs[-2:]
    terms, margins = refs[:count], refs[count:-2]
    half = min(term.shape[0] for term in terms) // 2 // 64 * 64
    quarter = half // 2
    if turned:
        keep_spots = ((0, quarter), (2 * quarter, quarter))
        send_spots = ((quarter, quarter), (3 * quarter, quarter))
    else:
        keep_spots, send_spots = ((0, half),), ((half, half),)
    for out_ref, spots in ((send_ref, send_spots), (keep_ref, keep_spots)):
        at = 0
        for first, rows in spots:
            total = terms[0][first : first + rows]
            for term in terms[1:]:
                total = total + term[first : first + rows]
            out_ref[at : at + rows] = total
            at += rows
        if margins:
            start = margins[0].shape[0] - EXTRA
            total = margins[0][start:]
            for margin in margins[1:]:
                total = total + margin[margin.shape[0] - EXTRA :]
            out_ref[half:] = total


def fold(terms, margins, turned):
    rows, width = min(term.shape for term in terms)
    half = rows // 2 // 64 * 64
    out = jax.ShapeDtypeStruct((half + (EXTRA if margins else 0), width), jnp.float32)
    return pl.pallas_call(
        functools.partial(fold_kernel, turned, len(terms)),
        out_shape=(out, out),
        in_specs=whole(len(terms) + len(margins)),
        compiler_params=params(8),
        name="fold",
    )(*terms, *margins)


def finish_kernel(sample_count, where_ref, *refs):
    total_hbm, allelic_hbm, total_ref, allelic_ref, sems = refs[-5:]
    own = total_ref.shape[0]
    samp = where_ref[0]
    chunks = len(CHUNKS)
    couples = [refs[at : at + 2] for at in range(0, 6 * chunks, 2)]
    pair_of = [couples[index * chunks : (index + 1) * chunks] for index in range(3)]
    left, right = pair_of[RIDE[0]][RIDE[1]]
    margin = left[own:, :] + right[own:, :]
    stride = CHUNKS[RIDE[1]]
    columns = []
    for kind in range(2):
        picked = jnp.zeros((1, LANES), jnp.float32)
        for source in range(lax.axis_size("var")):
            spot = 2 * source + kind
            row, block = 2 * chunks + spot // stride, spot % stride
            row_now = margin[row : row + 1, block * LANES : (block + 1) * LANES]
            picked = jnp.where(samp >> 1 == source, row_now, picked)
        turned = jnp.broadcast_to(picked, (LANES, LANES)).T
        columns.append(jnp.where(samp & 1 == 0, turned[:own], turned[own:]))
    dos_sum, dos_sq = columns
    dos_mean = dos_sum / sample_count
    dosage_var = dos_sq - dos_sum * dos_mean
    dos_scale = jnp.sqrt(jnp.float32(sample_count)) * lax.rsqrt(dosage_var + 1.0)
    first, copies = 0, []
    for chunk, blocks in enumerate(CHUNKS):
        for block in range(blocks):
            lanes = slice(block * LANES, (block + 1) * LANES)
            spot = slice((first + block) * LANES, (first + block + 1) * LANES)
            gene_sum = margin[2 * chunk : 2 * chunk + 1, lanes]
            gene_sq = margin[2 * chunk + 1 : 2 * chunk + 2, lanes]
            gene_var = gene_sq - gene_sum * gene_sum / sample_count
            pair_sums = [
                pair_of[index][chunk][0][:own, lanes] + pair_of[index][chunk][1][:own, lanes]
                for index in range(3)
            ]
            covariance = pair_sums[0] - dos_mean * gene_sum
            total_ref[:, spot] = covariance * dos_scale * lax.rsqrt(gene_var + 1.0)
            allelic_ref[:, spot] = pair_sums[1] * lax.rsqrt(pair_sums[2] + 1.0)
        lanes = pl.ds(first * LANES, blocks * LANES)
        for which, (ref, hbm) in enumerate(((total_ref, total_hbm), (allelic_ref, allelic_hbm))):
            copy = pltpu.make_async_copy(ref.at[:, lanes], hbm.at[:, lanes], sems.at[which, chunk])
            copy.start()
            copies.append(copy)
        first += blocks
    for copy in copies:
        copy.wait()


def finish(where, parts, own, width, sample_count):
    out = jax.ShapeDtypeStruct((own, width), jnp.float32)
    return pl.pallas_call(
        functools.partial(finish_kernel, sample_count),
        out_shape=(out, out),
        in_specs=[pl.BlockSpec(memory_space=pltpu.SMEM)] + whole(len(parts)),
        out_specs=(pl.BlockSpec(memory_space=pl.ANY),) * 2,
        scratch_shapes=[
            pltpu.VMEM((own, width), jnp.float32),
            pltpu.VMEM((own, width), jnp.float32),
            pltpu.SemaphoreType.DMA((2, len(CHUNKS))),
        ],
        compiler_params=params(8),
        name="finish",
    )(where, *parts)


def per_device(hap_words, total_counts, allele_one, allele_two):
    where = jnp.stack([lax.axis_index("samp"), lax.axis_index("var")]).astype(jnp.int32)
    twin = swap(hap_words, "var", 1)
    counts = (total_counts, allele_one, allele_two)
    made = []
    for call, blocks in enumerate(MADE):
        after = (twin,) if call else ()
        made.append(features(*counts, sum(MADE[:call]), blocks, after))
    pairs = [paired(hap_words, twin)]
    for flip in FAR:
        pairs.append(swap(pairs[0], "var", flip))
    *designs, dos_part = unpack(where, pairs)
    spots = [(call, block) for call, blocks in enumerate(MADE) for block in range(blocks)]
    kept, sent, came = {}, {}, {}
    for kind, index, chunk in PLAN:
        cell = index, chunk
        if kind in (SENDING, KEEPING):
            first = sum(CHUNKS[:chunk])
            mine = spots[first : first + CHUNKS[chunk]]
            calls = 1 + max(call for call, _ in mine)
            margins = []
            if cell == RIDE and kind == SENDING:
                margins = [*(parts[3] for parts in made), dos_part]
            features_of = [made[call][index] for call in range(calls)]
            part = int(kind == SENDING)
            keep, send = cross(designs[index], features_of, mine, part, margins)
        elif kind == FIRST:
            keep, send = None, meet(kept[SENDING, cell], came[SENDING, cell])
            sent[cell] = send
        elif kind == SECOND:
            terms = [kept[KEEPING, cell], came[KEEPING, cell], came[FIRST, cell]]
            margins = [sent[cell], came[FIRST, cell]] if cell == RIDE else []
            keep, send = fold(terms, margins, cell in TURNED)
        else:
            terms = [kept[SECOND, cell], came[SECOND, cell]]
            keep, send = fold(terms, terms if cell == RIDE else [], False)
        at = (FIRST, SECOND, THIRD).index(kind) if kind in (FIRST, SECOND, THIRD) else None
        side = CORE if at is None else sides(index, chunk)[at]
        kept[kind, cell], came[kind, cell] = keep, swap(send, "samp", side)
    sample_count = float(total_counts.shape[0] * lax.axis_size("samp"))
    own = designs[0].shape[0] // lax.axis_size("samp")
    parts = []
    for index in range(3):
        for chunk in range(len(CHUNKS)):
            parts += [kept[THIRD, (index, chunk)], came[THIRD, (index, chunk)]]
    return finish(where, parts, own, total_counts.shape[1], sample_count)


def solution(mesh):
    in_specs = (P(None, "samp", "var"), P("samp", "var"), P("samp", "var"), P("samp", "var"))
    out_specs = (P("samp", "var"), P("samp", "var"))

    return jax.shard_map(
        per_device, mesh=mesh, in_specs=in_specs, out_specs=out_specs, check_vma=False
    )
```

```python
import functools

import jax
import jax.numpy as jnp
from jax import lax
from jax.experimental import pallas as pl
from jax.experimental.pallas import tpu as pltpu
from jax.sharding import PartitionSpec as P

BITS = 30
HALF = BITS // 2
LANES = 128
MIB = 1024 * 1024
MADE = (2, 6)
CHUNKS = (4, 4)
RIDE = (0, 0)
EXTRA = 8

CORE, SIDE_Y, SIDE_A, SIDE_B = 1, 2, 4, 12
ORDERS = ((SIDE_Y, SIDE_A, SIDE_B), (SIDE_A, SIDE_B, SIDE_Y), (SIDE_B, SIDE_Y, SIDE_A))
TURNED = ()
SENDING, KEEPING, FIRST, SECOND, THIRD = "sending", "keeping", "first", "second", "third"
PLAN = (
    (SENDING, 1, 0),
    (SENDING, 0, 0),
    (SENDING, 2, 1),
    (FIRST, 1, 0),
    (FIRST, 0, 0),
    (FIRST, 2, 1),
    (SENDING, 1, 1),
    (SENDING, 0, 1),
    (SENDING, 2, 0),
    (KEEPING, 2, 1),
    (FIRST, 1, 1),
    (FIRST, 0, 1),
    (FIRST, 2, 0),
    (KEEPING, 1, 0),
    (KEEPING, 0, 0),
    (KEEPING, 0, 1),
    (SECOND, 0, 0),
    (SECOND, 1, 0),
    (KEEPING, 2, 0),
    (SECOND, 2, 1),
    (KEEPING, 1, 1),
    (SECOND, 0, 1),
    (SECOND, 2, 0),
    (SECOND, 1, 1),
    (THIRD, 0, 0),
    (THIRD, 2, 1),
    (THIRD, 1, 0),
    (THIRD, 0, 1),
    (THIRD, 2, 0),
    (THIRD, 1, 1),
)
FAR = (4, 2, 6)


def swap(array, axis, flip):
    size = lax.axis_size(axis)
    return lax.ppermute(array, axis, [(d, d ^ flip) for d in range(size)])


def place_of(relative, order):
    bits = {
        SIDE_Y: (relative >> 1) & 1,
        SIDE_A: ((relative >> 2) ^ (relative >> 3)) & 1,
        SIDE_B: (relative >> 3) & 1,
    }
    first, second, third = order
    return 8 * bits[first] + 4 * (relative & 1) + 2 * bits[second] + bits[third]


def sides(index, chunk):
    first, second, third = ORDERS[index]
    return (first, third, second) if (index, chunk) in TURNED else (first, second, third)


def whole(count):
    return [pl.BlockSpec(memory_space=pltpu.VMEM)] * count


def params(mib):
    return pltpu.CompilerParams(vmem_limit_bytes=mib * MIB)


def unpack_kernel(where_ref, *refs):
    word_refs = refs[:-6]
    dosage_ref, phase_ref, mixed_ref, margin_ref, wide_ref, mask_ref = refs[-6:]
    samp, var = where_ref[0], where_ref[1]
    low = (1 << HALF) - 1
    words, block = word_refs[0].shape[1:]
    rows = block // 2
    samples = float(words * BITS)
    one, zero = jnp.bfloat16(1), jnp.bfloat16(0)
    lane = lax.broadcasted_iota(jnp.int32, mask_ref.shape[1:], 1)
    for step in range(mask_ref.shape[0]):
        bits = jnp.where(lane < 2 * words, 1 << (2 * step), 2 << (2 * step))
        mask_ref[step] = bits.astype(jnp.int16)
    pieces = [
        (flip + twin, word_ref, 2 * twin)
        for flip, word_ref in zip((0, *FAR), word_refs)
        for twin in range(2)
    ]
    for flip, word_ref, spot in pieces:
        source = var ^ flip
        first, second = word_ref[spot], word_ref[spot + 1]
        ones = lax.population_count(first) + lax.population_count(second)
        mixed = lax.population_count(first ^ second)
        margin_ref[pl.ds(source, 1), 0:1, :] = (
            jnp.sum(ones.astype(jnp.float32), axis=0, keepdims=True) - samples
        )[None]
        margin_ref[pl.ds(source, 1), 1:2, :] = (
            samples - jnp.sum(mixed.astype(jnp.float32), axis=0, keepdims=True)
        )[None]
        turned = [
            jnp.concatenate([w & low, (w >> HALF) & low], axis=0).T.astype(jnp.int16)
            for w in (first, second)
        ]
        for part in range(2):
            relative = (2 * source + part) ^ samp
            starts = [pl.multiple_of(place_of(relative, order) * rows, rows) for order in ORDERS]
            mine = [t[part * rows : (part + 1) * rows] for t in turned]
            for hap, m in enumerate(mine):
                wide_ref[hap] = jnp.concatenate([m, m], axis=1)
            for bit in range(0, HALF, 2):
                both = min(2, HALF - bit)
                used = slice(0, both * 2 * words)
                mask = mask_ref[bit // 2, :, used]
                hap_one = jnp.where((wide_ref[0, :, used] & mask) != 0, one, zero)
                hap_two = jnp.where((wide_ref[1, :, used] & mask) != 0, one, zero)
                phase = hap_one - hap_two
                lanes = slice(bit * 2 * words, (bit + both) * 2 * words)
                dosage_ref[pl.ds(starts[0], rows), lanes] = (hap_one + hap_two) - one
                phase_ref[pl.ds(starts[1], rows), lanes] = phase
                mixed_ref[pl.ds(starts[2], rows), lanes] = phase * phase


def unpack(where, pairs):
    _, words, block = pairs[0].shape
    count = 2 * len(pairs)
    variants, samples = count * block, words * BITS
    design = jax.ShapeDtypeStruct((variants, samples), jnp.bfloat16)
    return pl.pallas_call(
        unpack_kernel,
        out_shape=(design,) * 3 + (jax.ShapeDtypeStruct((count, 2, block), jnp.float32),),
        in_specs=[pl.BlockSpec(memory_space=pltpu.SMEM)] + whole(len(pairs)),
        scratch_shapes=[
            pltpu.VMEM((2, block // 2, 4 * words), jnp.int16),
            pltpu.VMEM(((HALF + 1) // 2, block // 2, 4 * words), jnp.int16),
        ],
        cost_estimate=pl.CostEstimate(
            flops=6_000_000_000, bytes_accessed=6 * variants * samples, transcendentals=0
        ),
        compiler_params=params(8),
        name="unpack",
    )(where, *pairs)


def pair_kernel(own_ref, twin_ref, pair_ref):
    pair_ref[:2] = own_ref[...]
    pair_ref[2:] = twin_ref[...]


def paired(own, twin):
    _, words, block = own.shape
    return pl.pallas_call(
        pair_kernel,
        out_shape=jax.ShapeDtypeStruct((4, words, block), own.dtype),
        in_specs=whole(2),
        compiler_params=params(8),
        name="paired",
    )(own, twin)


def feature_kernel(first, total_hbm, one_hbm, two_hbm, *refs):
    total_out, weighted_out, weight_out, margin_ref, buffer, sems = refs[-6:]
    blocks, samples = total_out.shape[:2]
    words = samples // BITS

    pieces = [(block, 0, words) for block in range(blocks - 1)]
    pieces += [(blocks - 1, at, words // 2) for at in (0, words // 2)]

    def copies(piece):
        block, at, count = pieces[piece]
        lanes = pl.ds((first + block) * LANES, LANES)
        rows = pl.ds(at * BITS, count * BITS)
        return [
            pltpu.make_async_copy(
                ref.at[rows, lanes], buffer.at[spot, block, rows], sems.at[spot, piece]
            )
            for spot, ref in enumerate((total_hbm, one_hbm, two_hbm))
        ]

    for piece in range(len(pieces)):
        for copy in copies(piece):
            copy.start()
    for piece, (block, at, count) in enumerate(pieces):
        for copy in copies(piece):
            copy.wait()

        def step(bit, sums, block=block, at=at, count=count):
            log_sum, log_sq = sums
            for half in range(2):
                rows = pl.ds(bit + half * HALF + at * BITS, count, stride=BITS)
                start = (2 * bit + half) * words + at
                spot = pl.ds(pl.multiple_of(start, count), count)
                log_total = jnp.log(buffer[0, block, rows, :].astype(jnp.float32) + 1.0)
                one_plus = buffer[1, block, rows, :].astype(jnp.float32) + 1.0
                two_plus = buffer[2, block, rows, :].astype(jnp.float32) + 1.0
                log_ratio = jnp.log(one_plus / two_plus)
                weight = (one_plus * two_plus) / (one_plus + two_plus)
                total_out[block, spot, :] = log_total.astype(jnp.bfloat16)
                weighted_out[block, spot, :] = (weight * log_ratio).astype(jnp.bfloat16)
                weight_out[block, spot, :] = weight.astype(jnp.bfloat16)
                folded = log_total.reshape(count // 8, 8, LANES)
                log_sum = log_sum + jnp.sum(folded, axis=0)
                log_sq = log_sq + jnp.sum(folded * folded, axis=0)
            return log_sum, log_sq

        blank = jnp.zeros((8, LANES), jnp.float32)
        sums = lax.fori_loop(0, HALF, step, (blank, blank), unroll=3)
        for kind in range(2):
            spot = (slice(kind, kind + 1), slice(block * LANES, (block + 1) * LANES))
            total = jnp.sum(sums[kind], axis=0, keepdims=True)
            margin_ref[spot] = total + margin_ref[spot] if at else total


def features(total_counts, allele_one, allele_two, first, blocks, after):
    samples = total_counts.shape[0]
    width = blocks * LANES
    feature = jax.ShapeDtypeStruct((blocks, samples, LANES), jnp.bfloat16)
    return pl.pallas_call(
        functools.partial(feature_kernel, first),
        out_shape=(feature,) * 3 + (jax.ShapeDtypeStruct((2, width), jnp.float32),),
        in_specs=[pl.BlockSpec(memory_space=pltpu.HBM)] * 3
        + [pl.BlockSpec(memory_space=pl.ANY)] * len(after),
        out_specs=tuple(whole(4)),
        scratch_shapes=[
            pltpu.VMEM((3, blocks, samples, LANES), jnp.int32),
            pltpu.SemaphoreType.DMA((3, blocks + 1)),
        ],
        cost_estimate=pl.CostEstimate(
            flops=12_000_000 * width, bytes_accessed=18 * samples * width, transcendentals=0
        ),
        compiler_params=params(44),
        name="features",
    )(total_counts, allele_one, allele_two, *after)


def margin_rows(place, margin_refs):
    *gene_refs, dos_ref = margin_refs
    rows, first = [], 0
    for blocks in CHUNKS:
        call = 0
        at = first + place
        while at >= MADE[call]:
            at -= MADE[call]
            call += 1
        rows.append(gene_refs[call][:, at * LANES : (at + 1) * LANES])
        first += blocks
    stride = CHUNKS[RIDE[1]]
    for spot in range(place, 2 * dos_ref.shape[0], stride):
        rows.append(dos_ref[spot // 2, spot % 2 : spot % 2 + 1, :])
    return jnp.concatenate(rows, axis=0)


def cross_kernel(spots, part, margins, design_ref, *refs):
    keep_ref, send_ref = refs[-2:]
    calls = 1 + max(call for call, _ in spots)
    feature_refs, margin_refs = refs[:calls], refs[calls : calls + margins]
    half = design_ref.shape[0] // 2
    kept = half // 2
    for pair in range(len(spots) // 2):
        right = jnp.concatenate(
            [feature_refs[call][block] for call, block in spots[2 * pair : 2 * pair + 2]], axis=1
        )
        lanes = slice(pair * 2 * LANES, (pair + 1) * 2 * LANES)
        product = jnp.dot(
            design_ref[part * half : (part + 1) * half, :],
            right,
            preferred_element_type=jnp.float32,
        )
        keep_ref[:kept, lanes] = product[:kept]
        send_ref[:kept, lanes] = product[kept:]
    if margins:
        for place in range(len(spots)):
            rows = margin_rows(place, margin_refs)
            lanes = slice(place * LANES, (place + 1) * LANES)
            keep_ref[kept:, lanes] = rows
            send_ref[kept:, lanes] = rows


def cross(design, features_of, spots, part, margins):
    variants, samples = design.shape
    width = len(spots) * LANES
    rows = variants // 4 + (EXTRA if margins else 0)
    out = jax.ShapeDtypeStruct((rows, width), jnp.float32)
    return pl.pallas_call(
        functools.partial(cross_kernel, spots, part, len(margins)),
        out_shape=(out, out),
        in_specs=whole(1 + len(features_of) + len(margins)),
        cost_estimate=pl.CostEstimate(
            flops=variants * samples * width,
            bytes_accessed=2 * (variants + width) * samples,
            transcendentals=0,
        ),
        compiler_params=params(8),
        name="cross",
    )(design, *features_of, *margins)


def meet_kernel(left_ref, right_ref, out_ref):
    out_ref[...] = left_ref[...] + right_ref[...]


def meet(left, right):
    return pl.pallas_call(
        meet_kernel,
        out_shape=jax.ShapeDtypeStruct(left.shape, left.dtype),
        in_specs=whole(2),
        compiler_params=params(8),
        name="meet",
    )(left, right)


def fold_kernel(turned, count, *refs):
    keep_ref, send_ref = refs[-2:]
    terms, margins = refs[:count], refs[count:-2]
    half = min(term.shape[0] for term in terms) // 2 // 64 * 64
    quarter = half // 2
    if turned:
        keep_spots = ((0, quarter), (2 * quarter, quarter))
        send_spots = ((quarter, quarter), (3 * quarter, quarter))
    else:
        keep_spots, send_spots = ((0, half),), ((half, half),)
    for out_ref, spots in ((send_ref, send_spots), (keep_ref, keep_spots)):
        at = 0
        for first, rows in spots:
            total = terms[0][first : first + rows]
            for term in terms[1:]:
                total = total + term[first : first + rows]
            out_ref[at : at + rows] = total
            at += rows
        if margins:
            start = margins[0].shape[0] - EXTRA
            total = margins[0][start:]
            for margin in margins[1:]:
                total = total + margin[margin.shape[0] - EXTRA :]
            out_ref[half:] = total


def fold(terms, margins, turned):
    rows, width = min(term.shape for term in terms)
    half = rows // 2 // 64 * 64
    out = jax.ShapeDtypeStruct((half + (EXTRA if margins else 0), width), jnp.float32)
    return pl.pallas_call(
        functools.partial(fold_kernel, turned, len(terms)),
        out_shape=(out, out),
        in_specs=whole(len(terms) + len(margins)),
        compiler_params=params(8),
        name="fold",
    )(*terms, *margins)


def finish_kernel(sample_count, where_ref, *refs):
    total_hbm, allelic_hbm, total_ref, allelic_ref, sems = refs[-5:]
    own = total_ref.shape[0]
    samp = where_ref[0]
    chunks = len(CHUNKS)
    couples = [refs[at : at + 2] for at in range(0, 6 * chunks, 2)]
    pair_of = [couples[index * chunks : (index + 1) * chunks] for index in range(3)]
    left, right = pair_of[RIDE[0]][RIDE[1]]
    margin = left[own:, :] + right[own:, :]
    stride = CHUNKS[RIDE[1]]
    columns = []
    for kind in range(2):
        picked = jnp.zeros((1, LANES), jnp.float32)
        for source in range(lax.axis_size("var")):
            spot = 2 * source + kind
            row, block = 2 * chunks + spot // stride, spot % stride
            row_now = margin[row : row + 1, block * LANES : (block + 1) * LANES]
            picked = jnp.where(samp >> 1 == source, row_now, picked)
        turned = jnp.broadcast_to(picked, (LANES, LANES)).T
        columns.append(jnp.where(samp & 1 == 0, turned[:own], turned[own:]))
    dos_sum, dos_sq = columns
    dos_mean = dos_sum / sample_count
    dosage_var = dos_sq - dos_sum * dos_mean
    dos_scale = jnp.sqrt(jnp.float32(sample_count)) * lax.rsqrt(dosage_var + 1.0)
    first, copies = 0, []
    for chunk, blocks in enumerate(CHUNKS):
        for block in range(blocks):
            lanes = slice(block * LANES, (block + 1) * LANES)
            spot = slice((first + block) * LANES, (first + block + 1) * LANES)
            gene_sum = margin[2 * chunk : 2 * chunk + 1, lanes]
            gene_sq = margin[2 * chunk + 1 : 2 * chunk + 2, lanes]
            gene_var = gene_sq - gene_sum * gene_sum / sample_count
            pair_sums = [
                pair_of[index][chunk][0][:own, lanes] + pair_of[index][chunk][1][:own, lanes]
                for index in range(3)
            ]
            covariance = pair_sums[0] - dos_mean * gene_sum
            total_ref[:, spot] = covariance * dos_scale * lax.rsqrt(gene_var + 1.0)
            allelic_ref[:, spot] = pair_sums[1] * lax.rsqrt(pair_sums[2] + 1.0)
        lanes = pl.ds(first * LANES, blocks * LANES)
        for which, (ref, hbm) in enumerate(((total_ref, total_hbm), (allelic_ref, allelic_hbm))):
            copy = pltpu.make_async_copy(ref.at[:, lanes], hbm.at[:, lanes], sems.at[which, chunk])
            copy.start()
            copies.append(copy)
        first += blocks
    for copy in copies:
        copy.wait()


def finish(where, parts, own, width, sample_count):
    out = jax.ShapeDtypeStruct((own, width), jnp.float32)
    return pl.pallas_call(
        functools.partial(finish_kernel, sample_count),
        out_shape=(out, out),
        in_specs=[pl.BlockSpec(memory_space=pltpu.SMEM)] + whole(len(parts)),
        out_specs=(pl.BlockSpec(memory_space=pl.ANY),) * 2,
        scratch_shapes=[
            pltpu.VMEM((own, width), jnp.float32),
            pltpu.VMEM((own, width), jnp.float32),
            pltpu.SemaphoreType.DMA((2, len(CHUNKS))),
        ],
        compiler_params=params(8),
        name="finish",
    )(where, *parts)


def per_device(hap_words, total_counts, allele_one, allele_two):
    where = jnp.stack([lax.axis_index("samp"), lax.axis_index("var")]).astype(jnp.int32)
    twin = swap(hap_words, "var", 1)
    counts = (total_counts, allele_one, allele_two)
    made = []
    for call, blocks in enumerate(MADE):
        after = (twin,) if call else ()
        made.append(features(*counts, sum(MADE[:call]), blocks, after))
    pairs = [paired(hap_words, twin)]
    for flip in FAR:
        pairs.append(swap(pairs[0], "var", flip))
    *designs, dos_part = unpack(where, pairs)
    spots = [(call, block) for call, blocks in enumerate(MADE) for block in range(blocks)]
    kept, sent, came = {}, {}, {}
    for kind, index, chunk in PLAN:
        cell = index, chunk
        if kind in (SENDING, KEEPING):
            first = sum(CHUNKS[:chunk])
            mine = spots[first : first + CHUNKS[chunk]]
            calls = 1 + max(call for call, _ in mine)
            margins = []
            if cell == RIDE and kind == SENDING:
                margins = [*(parts[3] for parts in made), dos_part]
            features_of = [made[call][index] for call in range(calls)]
            part = int(kind == SENDING)
            keep, send = cross(designs[index], features_of, mine, part, margins)
        elif kind == FIRST:
            keep, send = None, meet(kept[SENDING, cell], came[SENDING, cell])
            sent[cell] = send
        elif kind == SECOND:
            terms = [kept[KEEPING, cell], came[KEEPING, cell], came[FIRST, cell]]
            margins = [sent[cell], came[FIRST, cell]] if cell == RIDE else []
            keep, send = fold(terms, margins, cell in TURNED)
        else:
            terms = [kept[SECOND, cell], came[SECOND, cell]]
            keep, send = fold(terms, terms if cell == RIDE else [], False)
        at = (FIRST, SECOND, THIRD).index(kind) if kind in (FIRST, SECOND, THIRD) else None
        side = CORE if at is None else sides(index, chunk)[at]
        kept[kind, cell], came[kind, cell] = keep, swap(send, "samp", side)
    sample_count = float(total_counts.shape[0] * lax.axis_size("samp"))
    own = designs[0].shape[0] // lax.axis_size("samp")
    parts = []
    for index in range(3):
        for chunk in range(len(CHUNKS)):
            parts += [kept[THIRD, (index, chunk)], came[THIRD, (index, chunk)]]
    return finish(where, parts, own, total_counts.shape[1], sample_count)


def solution(mesh):
    in_specs = (P(None, "samp", "var"), P("samp", "var"), P("samp", "var"), P("samp", "var"))
    out_specs = (P("samp", "var"), P("samp", "var"))

    return jax.shard_map(
        per_device, mesh=mesh, in_specs=in_specs, out_specs=out_specs, check_vma=False
    )
```
